32 devices in a mesh: seq: 16 (over z, y, core), head: 2 (over x).
Axes of the slice: x: 2, y: 2, z: 4, core: 2. Of those that a mesh axis runs over, the one named last changes fastest.
Arguments:
- image_in: bfloat16 [16384, 768], P(('seq', 'head')), may hold values from -6 to 6
- ln_gain: float32 [768], replicated, may hold values from 0.5 to 1.5
- w_in: bfloat16 [768, 5376], replicated, may hold values from -0.21875 to 0.21875
- q_gain: float32 [64], replicated, may hold values from 0.8 to 1.6
- k_gain: float32 [64], replicated, may hold values from 0.8 to 1.6
- w_attn_out: bfloat16 [768, 768], replicated, may hold values from -0.75 to 0.75
- w_mlp_out: bfloat16 [3072, 768], replicated, may hold values from -0.109375 to 0.109375
- cotangent: bfloat16 [16384, 768], P(('seq', 'head')), may hold values from -6 to 6
- image_ids: int32 [16, 1024], P('seq'), may hold values from 0 to 15, never falling along the last dimension, each value on 1 to 768 neighbouring positions
Outputs:
- block_out: bfloat16 [16384, 768], P(('seq', 'head'))
- grad_image: float32 [16384, 768], P(('seq', 'head'))
- grad_ln_gain: float32 [768], replicated
- grad_w_in: float32 [768, 5376], replicated
- grad_q_gain: float32 [64], replicated
- grad_k_gain: float32 [64], replicated
- grad_w_attn_out: float32 [768, 768], replicated
- grad_w_mlp_out: float32 [3072, 768], replicated
The draws below stay inside these ranges and needn't reach their ends.
Inputs may be any that keep to these rules, and one draw needn't show every extreme that they name: `image_ids`: along each row the ids never fall; the tokens of one image form a run of equal ids within one row; an image has 1 to 768 tokens, and in each row one image has exactly 768.
All inputs are finite; a program needn't handle non-finite values.
Results may differ from the reference program's by a relative error of at most 0.012.
Values may be sent and summed in bfloat16 or wider, within the bound.
No kernel may reach another device: no remote copies, remote signals or barrier semaphores. Data moves between devices by JAX's collectives and lax.ppermute only.
A program may use at most 192 MiB of HBM per device.

```python
import math
import jax
import jax.numpy as jnp
import numpy as np
from jax import lax

D = 768
HEADS = 12
HEAD_DIM = 64
MLP = 3072
GROUP_TOK = 1024
TOKENS = 16384
N_SEQ = 16


def levels(key, shape, pieces, least, high):
    def one(dim, shards_of):
        steps = jax.random.uniform(jax.random.fold_in(jax.random.fold_in(key, 6), dim), (shards_of,), jnp.float32, least / len(pieces), high / len(pieces))
        return jnp.repeat(jnp.exp(steps), shape[dim] // shards_of).reshape((-1,) + (1,) * (len(shape) - dim - 1))

    factor_of = one(*pieces[0])
    for cut in pieces[1:]:
        factor_of = factor_of * one(*cut)
    return factor_of


def length_profile(amount, total, bound, slope):
    weights = [(1 << 20) // math.isqrt(standing ** slope) + 1 for standing in range(2, amount + 1)]
    rest, given = total - bound - (amount - 1), [1] * (amount - 1)
    while rest > 0:
        free = [i for i in range(amount - 1) if given[i] < bound]
        whole, left = sum([weights[i] for i in free]), rest
        for i in free:
            extra = min(bound - given[i], max(1, left * weights[i] // whole), rest)
            given[i] = given[i] + extra
            rest = rest - extra
    return np.array([bound] + given)


def uneven(rng, number_of, total, most, slope):
    if number_of == 2:
        one = jax.random.randint(rng, (), max(1, total - most), min(most, total - 1) + 1)
        return jnp.stack([one, total - one])
    sizes = jnp.asarray(length_profile(number_of, total, most, slope), jnp.int32)
    pairs = (number_of - 1) // 2
    source_of, sink = sizes[1:1 + 2 * pairs:2], sizes[2:2 + 2 * pairs:2]
    slack = jnp.minimum(source_of - 1, most - sink)
    moved = jax.random.randint(jax.random.fold_in(rng, 1), (pairs,), 0, 1 << 20) % (slack + 1)
    sizes = sizes.at[1:1 + 2 * pairs:2].set(source_of - moved).at[2:2 + 2 * pairs:2].set(sink + moved)
    return sizes[jax.random.permutation(jax.random.fold_in(rng, 2), number_of)]


def normal_values(key, shape, width, bound, pieces=(), held_as=jnp.bfloat16):
    values = width * jax.random.normal(key, shape, jnp.float32)
    if pieces:
        values = values * levels(key, shape, pieces, -0.22, 0.18)
    return jnp.clip(values, -bound, bound).astype(held_as)


def setup_inputs(seed: int = 0) -> dict:
    splits = jax.random.split(jax.random.key(seed), 10)
    return {
        "image_in": normal_values(splits[0], (TOKENS, D), 1.0, 6.0, ((0, 32),)),
        "ln_gain": jnp.clip(jax.random.uniform(splits[1], (D,), jnp.float32, 0.5, 1.5), 0.5, 1.5),
        "w_in": normal_values(splits[2], (D, 3 * HEADS * HEAD_DIM + MLP), D ** -0.5, 0.21875),
        "q_gain": jnp.clip(jax.random.uniform(splits[3], (HEAD_DIM,), jnp.float32, 0.8, 1.6), 0.8, 1.6),
        "k_gain": jnp.clip(jax.random.uniform(splits[4], (HEAD_DIM,), jnp.float32, 0.8, 1.6), 0.8, 1.6),
        "w_attn_out": normal_values(splits[5], (HEADS * HEAD_DIM, D), HEAD_DIM ** -0.5, 0.75),
        "w_mlp_out": normal_values(splits[6], (MLP, D), MLP ** -0.5, 0.109375),
        "cotangent": normal_values(splits[7], (TOKENS, D), 1.0, 6.0, ((0, 32),)),
        "image_ids": jax.vmap(lambda own: jnp.searchsorted(jnp.cumsum(uneven(own, max(3, GROUP_TOK // 64), GROUP_TOK, 3 * GROUP_TOK // 4, 2)), jnp.arange(GROUP_TOK), side="right"))(jax.random.split(splits[8], N_SEQ)).reshape((N_SEQ, GROUP_TOK)).astype(jnp.int32),
    }


@jax.custom_vjp
def low(v):
    return lax.optimization_barrier(v.astype(jnp.bfloat16)).astype(jnp.float32)

@jax.custom_vjp
def low_back(v):
    return v

def low_keep(v):
    return (low(v), None)

def low_pass(kept, grad):
    return (grad,)

def back_keep(v):
    return (v, None)

def back_low(kept, grad):
    return (low(grad),)
low.defvjp(low_keep, low_pass)
low_back.defvjp(back_keep, back_low)
norm_epsilon = 1e-06
highest = lax.Precision.HIGHEST

def norm_rows(values, gain):
    center = values - lax.optimization_barrier(jnp.mean(values, axis=-1, keepdims=True))
    spread = lax.optimization_barrier(jnp.mean(center * center, axis=-1, keepdims=True))
    return center * lax.rsqrt(spread + norm_epsilon) * gain

def attend_block(query_rows, id_rows, keys_all, values_all, ids_all):
    raw_scores = jnp.einsum('rhe,ghe->hrg', query_rows, keys_all, precision=highest) * 0.125
    scores = low_back(raw_scores)
    same_image = id_rows[:, None] == ids_all[None, :]
    masked = jnp.where(same_image[None], scores, -1e+30)
    weights = low(jax.nn.softmax(masked, axis=-1))
    return jnp.einsum('hrg,ghe->rhe', weights, values_all, precision=highest)

def group_attention(qkv_group, id_row, q_gain, k_gain):
    queries = low(norm_rows(qkv_group[:, 0], q_gain))
    keys_all = low(norm_rows(qkv_group[:, 1], k_gain))
    values_all = qkv_group[:, 2]
    block_rows = min(512, GROUP_TOK)
    block_count = GROUP_TOK // block_rows
    query_blocks = queries.reshape(block_count, block_rows, HEADS, HEAD_DIM)
    id_blocks = id_row.reshape(block_count, block_rows)
    checked = jax.checkpoint(attend_block)

    def one_block(block_pair):
        return checked(block_pair[0], block_pair[1], keys_all, values_all, id_row)
    attended = lax.map(one_block, (query_blocks, id_blocks))
    return attended.reshape(GROUP_TOK, HEADS * HEAD_DIM)

def forward(image_in, ln_gain, w_in, q_gain, k_gain, w_attn_out, w_mlp_out, image_ids):
    normed = low(norm_rows(image_in, ln_gain))
    proj = jnp.dot(normed, w_in, precision=highest)
    span = HEADS * HEAD_DIM
    qkv = low_back(low(proj[:, :3 * span]))
    upper = low_back(proj[:, 3 * span:])
    act = low(jax.nn.gelu(upper, approximate=False))
    groups = qkv.reshape(N_SEQ, GROUP_TOK, 3, HEADS, HEAD_DIM)

    def one_group(group_pair):
        return group_attention(group_pair[0], group_pair[1], q_gain, k_gain)
    attended = lax.map(one_group, (groups, image_ids)).reshape(TOKENS, span)
    attended = low_back(low(attended))
    branch = jnp.dot(attended, w_attn_out, precision=highest) + jnp.dot(act, w_mlp_out, precision=highest)
    return image_in + branch

def reference(image_in, ln_gain, w_in, q_gain, k_gain, w_attn_out, w_mlp_out, cotangent, image_ids):

    def wrapped(image_f32, ln_f32, w_in_f32, q_f32, k_f32, attn_f32, mlp_f32):
        return forward(image_f32, ln_f32, w_in_f32, q_f32, k_f32, attn_f32, mlp_f32, image_ids)
    result, pull = jax.vjp(wrapped, image_in.astype(jnp.float32), ln_gain.astype(jnp.float32), w_in.astype(jnp.float32), q_gain.astype(jnp.float32), k_gain.astype(jnp.float32), w_attn_out.astype(jnp.float32), w_mlp_out.astype(jnp.float32))
    grads = pull(cotangent.astype(jnp.float32))
    return (result.astype(jnp.bfloat16), grads[0], grads[1], grads[2], grads[3], grads[4], grads[5], grads[6])
```

```python
import functools
import math

import jax
import jax.numpy as jnp
from jax import lax
from jax.experimental import pallas as pl
from jax.experimental.pallas import tpu as pltpu
from jax.sharding import PartitionSpec as P

F32 = jnp.float32
BF16 = jnp.bfloat16
EPS = 1e-06
AXES = ("seq", "head")
BLOCKS = 16
EXCLUDE = 32768.0
SCORE_SCALE = 0.125 * math.log2(math.e)


def dot_nn(a, b):
    return lax.dot_general(a, b, (((1,), (0,)), ((), ())), preferred_element_type=F32)


def dot_nt(a, b):
    return lax.dot_general(a, b, (((1,), (1,)), ((), ())), preferred_element_type=F32)


def dot_tn(a, b):
    return lax.dot_general(a, b, (((0,), (0,)), ((), ())), preferred_element_type=F32)


def prep_body(ids_ref, image_ref, cot_ref, gain_ref, out_ref):
    tokens, width = image_ref.shape
    step = 64
    for r in range(0, tokens, step):
        x = image_ref[r : r + step, :].astype(F32)
        center = x - jnp.mean(x, axis=-1, keepdims=True)
        spread = jnp.mean(center * center, axis=-1, keepdims=True)
        out_ref[r : r + step, 0:width] = (center * lax.rsqrt(spread + EPS) * gain_ref[...]).astype(BF16)
    out_ref[:, width : 2 * width] = cot_ref[...]
    ids = ids_ref[...]
    image = lax.broadcasted_iota(jnp.int32, (128, tokens), 0) & 63
    marks = jnp.where(image == ids, 1.0, 0.0).astype(F32)
    out_ref[:, 2 * width :] = jnp.transpose(marks).astype(BF16)


def prep(ids, image_in, cotangent, ln_gain):
    tokens, width = image_in.shape
    return pl.pallas_call(
        prep_body,
        out_shape=jax.ShapeDtypeStruct((tokens, 2 * width + 128), BF16),
        cost_estimate=pl.CostEstimate(flops=10 * tokens * width, bytes_accessed=8 * tokens * width, transcendentals=0),
        name="prep",
    )(ids, image_in, cotangent, ln_gain)


def mlp_body(pos_ref, normed_ref, cot_ref, win_ref, wout_ref, grads_ref, bo_ref, dn_ref, up_s, dact_s, act_s, dup_s):
    tokens, width = normed_ref.shape
    sid = pos_ref[1]
    up_s[...] = dot_nn(normed_ref[...], win_ref[...])
    dact_s[...] = dot_nt(cot_ref[...], wout_ref[...])
    step = 32

    def gelu_rows(i, carry):
        rows = pl.ds(pl.multiple_of(i * step, step), step)
        up = up_s[rows, :]
        cdf = 0.5 * (1.0 + lax.erf(up * math.sqrt(0.5)))
        pdf = jnp.exp(-0.5 * up * up) * (1.0 / math.sqrt(2.0 * math.pi))
        act_s[rows, :] = (up * cdf).astype(BF16)
        dup_s[rows, :] = (dact_s[rows, :] * (cdf + up * pdf)).astype(BF16)
        return carry

    lax.fori_loop(0, tokens // step, gelu_rows, 0)
    rows = width // BLOCKS
    part = 384
    for j in range(0, width, part):
        grad_out = dot_tn(act_s[:, j : j + part], cot_ref[...])
        grad_in = dot_tn(normed_ref[:, j : j + part], dup_s[...])
        for i in range(part // rows):
            where = (j // rows + i) ^ sid
            grads_ref[0, where, 0:rows, :] = grad_out[i * rows : (i + 1) * rows].astype(BF16)
            grads_ref[0, where, rows : 2 * rows, :] = grad_in[i * rows : (i + 1) * rows].astype(BF16)
    first = pl.program_id(0) == 0
    bo = dot_nn(act_s[...], wout_ref[...])
    dn = dot_nt(dup_s[...], win_ref[...])

    @pl.when(first)
    def _():
        bo_ref[...] = bo
        dn_ref[...] = dn

    @pl.when(jnp.logical_not(first))
    def _():
        bo_ref[...] += bo
        dn_ref[...] += dn


def mlp(pos, packed, w_in, w_mlp_out, part):
    tokens = packed.shape[0]
    width = w_mlp_out.shape[1]
    rows = width // BLOCKS
    first = 3 + 2 * part
    return pl.pallas_call(
        mlp_body,
        out_shape=(
            jax.ShapeDtypeStruct((2, BLOCKS, 2 * rows, width), BF16),
            jax.ShapeDtypeStruct((tokens, width), F32),
            jax.ShapeDtypeStruct((tokens, width), F32),
        ),
        grid_spec=pltpu.PrefetchScalarGridSpec(
            num_scalar_prefetch=1,
            grid=(2,),
            in_specs=[
                pl.BlockSpec((tokens, width), lambda t, pos: (0, 0)),
                pl.BlockSpec((tokens, width), lambda t, pos: (0, 1)),
                pl.BlockSpec((width, width), lambda t, pos: (0, first + t)),
                pl.BlockSpec((width, width), lambda t, pos: (2 * part + t, 0)),
            ],
            out_specs=[
                pl.BlockSpec((1, BLOCKS, 2 * rows, width), lambda t, pos: (t ^ pos[0], 0, 0, 0)),
                pl.BlockSpec((tokens, width), lambda t, pos: (0, 0)),
                pl.BlockSpec((tokens, width), lambda t, pos: (0, 0)),
            ],
            scratch_shapes=[
                pltpu.VMEM((tokens, width), F32),
                pltpu.VMEM((tokens, width), F32),
                pltpu.VMEM((tokens, width), BF16),
                pltpu.VMEM((tokens, width), BF16),
            ],
        ),
        compiler_params=pltpu.CompilerParams(dimension_semantics=("arbitrary",)),
        cost_estimate=pl.CostEstimate(
            flops=2 * 6 * 2 * tokens * width * width, bytes_accessed=16 * width * width, transcendentals=4 * tokens * width
        ),
        name=f"mlp{part}",
    )(pos, packed, packed, w_in, w_mlp_out)


def half_sums(x, low):
    left = jnp.sum(jnp.where(low, x, 0.0), axis=-1, keepdims=True)
    right = jnp.sum(jnp.where(low, 0.0, x), axis=-1, keepdims=True)
    return jnp.where(low, left, right)


def head_norm(x, low, size):
    center = x - half_sums(x, low) * (1.0 / size)
    rstd = lax.rsqrt(half_sums(center * center, low) * (1.0 / size) + EPS)
    return center * rstd, rstd


def attention_body(
    pos_ref, own_ref, mate_ref, wq_ref, wk_ref, wv_ref, wo_ref, gq_ref, gk_ref,
    grads_ref, gains_ref, part_ref,
    w_s, raw_s, dout_s, q_s, k_s, v_s, dq_s, dk_s, dv_s, att_s, dproj_s, bo_s, dn_s,
):
    tokens = own_ref.shape[0]
    width = wo_ref.shape[1]
    group = 2 * tokens
    size = 64
    pair = pl.program_id(0)
    sid = pos_ref[1]
    w_s[:, 0:128] = wq_ref[...]
    w_s[:, 128:256] = wk_ref[...]
    w_s[:, 256:384] = wv_ref[...]
    halves = ((0, own_ref), (tokens, mate_ref))
    for r, ref in halves:
        raw_s[r : r + tokens, :] = dot_nn(ref[:, 0:width], w_s[...]).astype(BF16)
        dout_s[r : r + tokens, :] = dot_nt(ref[:, width : 2 * width], wo_ref[...]).astype(BF16)

    step = 128

    def lanes(rows):
        return lax.broadcasted_iota(jnp.int32, (rows, 128), 1)

    for r, ref in halves:

        def norm_rows(i, carry, r=r, ref=ref):
            here = pl.ds(pl.multiple_of(i * step, step), step)
            rows = pl.ds(pl.multiple_of(r + i * step, step), step)
            low = lanes(step) < size
            marks = ref[here, 2 * width :].astype(F32)
            qn = head_norm(raw_s[rows, 0:128].astype(F32), low, size)[0] * gq_ref[...]
            kn = head_norm(raw_s[rows, 128:256].astype(F32), low, size)[0] * gk_ref[...]
            v = raw_s[rows, 256:384].astype(F32)
            away = (marks - 1.0) * EXCLUDE
            for h in range(2):
                mine = low if h == 0 else jnp.logical_not(low)
                q_s[h, rows, :] = jnp.where(mine, qn, marks).astype(BF16)
                k_s[h, rows, :] = jnp.where(mine, kn, away).astype(BF16)
                v_s[h, rows, :] = jnp.where(mine, v, 1.0).astype(BF16)
            return carry

        lax.fori_loop(0, tokens // step, norm_rows, 0)

    block = 256
    dk_s[...] = jnp.zeros_like(dk_s)
    dv_s[...] = jnp.zeros_like(dv_s)

    def query_block(i, carry):
        rows = pl.ds(pl.multiple_of(i * block, block), block)
        lane = lanes(block)
        low = lane < size
        for h in range(2):
            mine = low if h == 0 else jnp.logical_not(low)
            spare = size if h == 0 else 0
            q = q_s[h, rows, :]
            expd = jnp.exp2(dot_nt(q, k_s[h]) * SCORE_SCALE)
            expd_low = expd.astype(BF16)
            outs = dot_nn(expd_low, v_s[h])
            inverse = 1.0 / pltpu.roll(outs, size, 1)
            attended = outs * inverse
            grad = dout_s[rows, :].astype(F32) * inverse
            grad_low = grad.astype(BF16).astype(F32)
            centre = jnp.sum(jnp.where(mine, grad_low * attended, 0.0), axis=-1, keepdims=True)
            centre_high = centre.astype(BF16).astype(F32)
            extra = jnp.where(lane == spare, -centre_high, jnp.where(lane == spare + 1, centre_high - centre, 0.0))
            grad_ext = jnp.where(mine, grad_low, extra).astype(BF16)
            d_scores = (expd * dot_nt(grad_ext, v_s[h])).astype(BF16)
            dv_s[h] += dot_tn(expd_low, grad_ext)
            dk_s[h] += dot_tn(d_scores, q)
            dq = dot_nn(d_scores, k_s[h])
            if h == 0:
                att_s[rows, :] = attended
                dq_s[rows, :] = dq
            else:
                att_s[rows, :] = jnp.where(mine, attended, att_s[rows, :])
                dq_s[rows, :] = jnp.where(mine, dq, dq_s[rows, :])
        return carry

    lax.fori_loop(0, group // block, query_block, 0)

    @pl.when(pair == 0)
    def _():
        gains_ref[...] = jnp.zeros_like(gains_ref)

    def norm_back(i, carry):
        rows = pl.ds(pl.multiple_of(i * step, step), step)
        low = lanes(step) < size
        grads = (dq_s[rows, :], jnp.where(low, dk_s[0, rows, :], dk_s[1, rows, :]))
        for n, (grad, gain_ref) in enumerate(zip(grads, (gq_ref, gk_ref))):
            scaled, rstd = head_norm(raw_s[rows, 128 * n : 128 * (n + 1)].astype(F32), low, size)
            grad = grad * 0.125
            gains_ref[8 * n : 8 * (n + 1), :] += jnp.sum((grad * scaled).reshape(step // 8, 8, 128), axis=0)
            grad = grad * gain_ref[...]
            mean = half_sums(grad, low) * (1.0 / size)
            slope = half_sums(grad * scaled, low) * (1.0 / size)
            dproj_s[rows, 128 * n : 128 * (n + 1)] = (rstd * (grad - mean - scaled * slope)).astype(BF16)
        dproj_s[rows, 256:384] = jnp.where(low, dv_s[0, rows, :], dv_s[1, rows, :]).astype(BF16)
        return carry

    lax.fori_loop(0, group // step, norm_back, 0)

    rows = width // BLOCKS
    part = 384
    for j in range(0, width, part):
        grad_in = dot_tn(own_ref[:, j : j + part], dproj_s[0:tokens, :])
        grad_in += dot_tn(mate_ref[:, j : j + part], dproj_s[tokens:group, :])
        for i in range(part // rows):
            grads_ref[(j // rows + i) ^ sid, 0:rows, :] = grad_in[i * rows : (i + 1) * rows].astype(BF16)
    grad_out = dot_tn(att_s[0:tokens, :].astype(BF16), own_ref[:, width : 2 * width])
    grad_out += dot_tn(att_s[tokens:group, :].astype(BF16), mate_ref[:, width : 2 * width])
    few = 128 // BLOCKS
    for i in range(BLOCKS):
        piece = grad_out[i * few : (i + 1) * few]
        piece = jnp.concatenate([piece[:, :384], piece[:, 384:]], axis=0)
        grads_ref[i ^ sid, rows : rows + 2 * few, :] = piece.astype(BF16)

    bo = dot_nn(att_s[...].astype(BF16), wo_ref[...])
    dn = dot_nt(dproj_s[...], w_s[...])

    @pl.when(pair == 0)
    def _():
        bo_s[...] = bo
        dn_s[...] = dn

    @pl.when(pair == 1)
    def _():
        bo_s[...] += bo
        dn_s[...] += dn

    @pl.when(pair == 2)
    def _():
        for n in range(2):
            there = slice(n * tokens, (n + 1) * tokens)
            part_ref[n, :, 0:width] = (bo_s[there, :] + bo[there, :]).astype(BF16)
            part_ref[n, :, width : 2 * width] = (dn_s[there, :] + dn[there, :]).astype(BF16)


def attention(pos, own, mate, w_in, w_attn_out, gain_q, gain_k):
    tokens, packed = own.shape
    width = w_attn_out.shape[1]
    group = 2 * tokens
    rows = width // BLOCKS + 16
    whole = pl.BlockSpec((tokens, packed), lambda p, pos: (0, 0))
    gain = pl.BlockSpec((1, 128), lambda p, pos: (0, 0))
    return pl.pallas_call(
        attention_body,
        out_shape=(
            jax.ShapeDtypeStruct((BLOCKS, rows, 3 * 384), BF16),
            jax.ShapeDtypeStruct((16, 128), F32),
            jax.ShapeDtypeStruct((2, tokens, 2 * width), BF16),
        ),
        grid_spec=pltpu.PrefetchScalarGridSpec(
            num_scalar_prefetch=1,
            grid=(3,),
            in_specs=[
                whole,
                whole,
                pl.BlockSpec((width, 128), lambda p, pos: (0, 3 * pos[0] + p)),
                pl.BlockSpec((width, 128), lambda p, pos: (0, 6 + 3 * pos[0] + p)),
                pl.BlockSpec((width, 128), lambda p, pos: (0, 12 + 3 * pos[0] + p)),
                pl.BlockSpec((128, width), lambda p, pos: (3 * pos[0] + p, 0)),
                gain,
                gain,
            ],
            out_specs=[
                pl.BlockSpec((BLOCKS, rows, 384), lambda p, pos: (0, 0, p)),
                pl.BlockSpec((16, 128), lambda p, pos: (0, 0)),
                pl.BlockSpec((2, tokens, 2 * width), lambda p, pos: (0, 0, 0)),
            ],
            scratch_shapes=[
                pltpu.VMEM((width, 384), BF16),
                pltpu.VMEM((group, 384), BF16),
                pltpu.VMEM((group, 128), BF16),
                pltpu.VMEM((2, group, 128), BF16),
                pltpu.VMEM((2, group, 128), BF16),
                pltpu.VMEM((2, group, 128), BF16),
                pltpu.VMEM((group, 128), F32),
                pltpu.VMEM((2, group, 128), F32),
                pltpu.VMEM((2, group, 128), F32),
                pltpu.VMEM((group, 128), F32),
                pltpu.VMEM((group, 384), BF16),
                pltpu.VMEM((group, width), F32),
                pltpu.VMEM((group, width), F32),
            ],
        ),
        compiler_params=pltpu.CompilerParams(dimension_semantics=("arbitrary",)),
        cost_estimate=pl.CostEstimate(
            flops=6 * 6 * 2 * group * group * 128, bytes_accessed=16 * tokens * width, transcendentals=6 * group * group
        ),
        name="attention",
    )(pos, own, mate, w_in, w_in, w_in, w_attn_out, gain_q, gain_k)


def finish_body(image_ref, cot_ref, gain_ref, bo_ref, dn_ref, bo2_ref, dn2_ref, got_ref, out_ref, grad_ref, ln_ref):
    tokens, width = image_ref.shape
    step = 32
    ln_ref[...] = jnp.zeros_like(ln_ref)

    def some_rows(i, carry):
        rows = pl.ds(pl.multiple_of(i * step, step), step)
        x = image_ref[rows, :].astype(F32)
        got = got_ref[rows, :].astype(F32)
        out_ref[rows, :] = (x + (bo_ref[rows, :] + bo2_ref[rows, :] + got[:, 0:width])).astype(BF16)
        center = x - jnp.mean(x, axis=-1, keepdims=True)
        rstd = lax.rsqrt(jnp.mean(center * center, axis=-1, keepdims=True) + EPS)
        scaled = center * rstd
        grad = dn_ref[rows, :] + dn2_ref[rows, :] + got[:, width : 2 * width]
        ln_ref[...] += jnp.sum((grad * scaled).reshape(step // 8, 8, width), axis=0)
        grad = grad * gain_ref[...]
        mean = jnp.mean(grad, axis=-1, keepdims=True)
        slope = jnp.mean(grad * scaled, axis=-1, keepdims=True)
        grad_ref[rows, :] = cot_ref[rows, :].astype(F32) + rstd * (grad - mean - scaled * slope)
        return carry

    lax.fori_loop(0, tokens // step, some_rows, 0)


def finish(image_in, cotangent, ln_gain, bo, dn, bo2, dn2, got):
    tokens, width = image_in.shape
    return pl.pallas_call(
        finish_body,
        out_shape=(
            jax.ShapeDtypeStruct((tokens, width), BF16),
            jax.ShapeDtypeStruct((tokens, width), F32),
            jax.ShapeDtypeStruct((8, width), F32),
        ),
        cost_estimate=pl.CostEstimate(flops=30 * tokens * width, bytes_accessed=30 * tokens * width, transcendentals=0),
        name="finish",
    )(image_in, cotangent, ln_gain, bo, dn, bo2, dn2, got)


def exchange(value, mask):
    count = lax.axis_size(AXES)
    return lax.ppermute(value, AXES, [(i, i ^ mask) for i in range(count)])


def add_low(left, right):
    return (left.astype(F32) + right.astype(F32)).astype(BF16)


def reduce_scatter(chunk, masks, rest):
    for mask in masks:
        half = chunk.shape[0] // 2
        chunk = add_low(chunk[:half], exchange(chunk[half:], mask))
    for mask in rest:
        chunk = add_low(chunk, exchange(chunk, mask))
    return chunk


def all_gather(chunk, masks):
    for mask in reversed(masks):
        chunk = jnp.concatenate([chunk, exchange(chunk, mask)], axis=0)
    return chunk


def spread_mlp_body(pos_ref, own_ref, mate_ref, *refs):
    out_ref, in_ref = refs[-2:]
    sid = pos_ref[1]
    rows = own_ref.shape[1] // 2
    side, quarter = pl.program_id(0), pl.program_id(1)

    def put(source):
        for i in range(4):
            at = (4 * quarter + i) ^ sid
            out_ref[i * rows : (i + 1) * rows, :] = source[at, 0:rows, :].astype(F32)
            in_ref[i * rows : (i + 1) * rows, :] = source[at, rows : 2 * rows, :].astype(F32)

    pl.when(side == 0)(lambda: put(own_ref))
    pl.when(side == 1)(lambda: put(mate_ref))


def spread_mlp(pos, own, mate, part, shapes, before):
    blocks, rows2, width = own.shape
    whole = pl.BlockSpec(own.shape, lambda r, g, pos: (0, 0, 0))
    return pl.pallas_call(
        spread_mlp_body,
        out_shape=tuple(jax.ShapeDtypeStruct(s, F32) for s in shapes),
        grid_spec=pltpu.PrefetchScalarGridSpec(
            num_scalar_prefetch=1,
            grid=(2, 4),
            in_specs=[whole, whole] + [pl.BlockSpec(memory_space=pl.ANY)] * len(before),
            out_specs=[
                pl.BlockSpec((width // 4, width), lambda r, g, pos: (4 * (2 * part + (r ^ pos[0])) + g, 0)),
                pl.BlockSpec((width // 4, width), lambda r, g, pos: (g, 3 + 2 * part + (r ^ pos[0]))),
            ],
        ),
        input_output_aliases={3 + i: i for i in range(len(before))},
        compiler_params=pltpu.CompilerParams(dimension_semantics=("arbitrary", "arbitrary")),
        cost_estimate=pl.CostEstimate(flops=0, bytes_accessed=24 * width * width, transcendentals=0),
        name=f"spread_mlp{part}",
    )(pos, own, mate, *before)


def spread_attention_body(pos_ref, own_ref, mate_ref, _, in_ref, out_ref):
    sid = pos_ref[1]
    blocks = own_ref.shape[0]
    rows = own_ref.shape[1] - 16
    side, kind = pl.program_id(0), pl.program_id(1)

    def put(source):
        for i in range(blocks):
            at = i ^ sid
            for p in range(3):
                from_col = pl.ds(pl.multiple_of(384 * p + 128 * kind, 128), 128)
                in_ref[i * rows : (i + 1) * rows, 128 * p : 128 * (p + 1)] = source[at, 0:rows, from_col].astype(F32)

        @pl.when(kind == 0)
        def _():
            for i in range(blocks):
                at = i ^ sid
                for p in range(3):
                    piece = source[at, rows : rows + 16, 384 * p : 384 * (p + 1)].astype(F32)
                    to = slice(128 * p + 8 * i, 128 * p + 8 * (i + 1))
                    out_ref[to, 0:384] = piece[0:8]
                    out_ref[to, 384:768] = piece[8:16]

    pl.when(side == 0)(lambda: put(own_ref))
    pl.when(side == 1)(lambda: put(mate_ref))


def spread_attention(pos, own, mate, before, out_shape):
    whole = pl.BlockSpec(own.shape, lambda r, k, pos: (0, 0, 0))
    width = out_shape[0]
    return pl.pallas_call(
        spread_attention_body,
        out_shape=(jax.ShapeDtypeStruct(before.shape, F32), jax.ShapeDtypeStruct(out_shape, F32)),
        grid_spec=pltpu.PrefetchScalarGridSpec(
            num_scalar_prefetch=1,
            grid=(2, 3),
            in_specs=[whole, whole, pl.BlockSpec(memory_space=pl.ANY)],
            out_specs=[
                pl.BlockSpec((width, 384), lambda r, k, pos: (0, 2 * k + (r ^ pos[0]))),
                pl.BlockSpec((384, width), lambda r, k, pos: (r ^ pos[0], 0)),
            ],
        ),
        input_output_aliases={3: 0},
        compiler_params=pltpu.CompilerParams(dimension_semantics=("arbitrary", "arbitrary")),
        cost_estimate=pl.CostEstimate(flops=0, bytes_accessed=24 * width * width, transcendentals=0),
        name="spread_attention",
    )(pos, own, mate, before)


def per_device(image_in, ln_gain, w_in, q_gain, k_gain, w_attn_out, w_mlp_out, cotangent, image_ids):
    tokens, width = image_in.shape
    count = lax.axis_size(AXES)
    index = lax.axis_index(AXES)
    side = index & 1
    core = (index >> 1) & 1
    others = [1 << k for k in range(2, count.bit_length() - 1)]
    masks_x = [1] + others[:3]
    masks_y = [others[0], 1] + others[1:3]
    rest = others[3:]

    def place(masks):
        sid = jnp.int32(0)
        for mask in masks:
            sid = 2 * sid + ((index & mask) != 0).astype(jnp.int32)
        return jnp.stack([core, sid])

    pos_x, pos_y = place(masks_x), place(masks_y)
    gain_row = ln_gain.reshape(1, width)
    ids = lax.dynamic_slice(image_ids, (0, side * tokens), (1, tokens))
    packed = prep(ids, image_in, cotangent, gain_row)
    swapped = lax.ppermute(
        packed, AXES, [(i, (i & ~3) | ((i & 1) << 1) | ((i >> 1) & 1)) for i in range(count)]
    )
    grads0, bo0, dn0 = mlp(pos_x, packed, w_in, w_mlp_out, 0)
    mate = exchange(swapped, 2)
    grads1, bo1, dn1 = mlp(pos_y, packed, w_in, w_mlp_out, 1)

    def gather(chunk, masks):
        shard = reduce_scatter(chunk, masks, rest)
        own = all_gather(shard, masks)
        return own, exchange(own, 2)

    def pair_sum(grads):
        return add_low(grads[0], exchange(grads[1], 2))

    own0, mate0 = gather(pair_sum(grads0), masks_x)
    own1, mate1 = gather(pair_sum(grads1), masks_y)
    gain_q = jnp.concatenate([q_gain, q_gain]).reshape(1, 128)
    gain_k = jnp.concatenate([k_gain, k_gain]).reshape(1, 128)
    grads2, gains, parts = attention(pos_x, swapped, mate, w_in, w_attn_out, gain_q, gain_k)
    joined = add_low(parts[0], exchange(parts[1], 2))
    got = lax.ppermute(
        joined, AXES, [(i, (i & ~3) | ((i & 1) << 1) | ((i >> 1) & 1)) for i in range(count)]
    )
    own2, mate2 = gather(grads2, masks_x)
    block_out, grad_image, ln_part = finish(image_in, cotangent, gain_row, bo0, dn0, bo1, dn1, got)
    ln_row = jnp.sum(ln_part, axis=0)
    gain_rows = jnp.sum(gains.reshape(2, 8, 2, 64), axis=(1, 2))
    small = jnp.concatenate([ln_row, gain_rows.reshape(128), jnp.zeros((128,), F32)]).reshape(1, 8, 128)
    small = lax.all_to_all(jnp.broadcast_to(small, (count, 8, 128)), AXES, split_axis=0, concat_axis=0, tiled=True)
    small = jnp.sum(small, axis=0).reshape(1024)
    shapes = (w_mlp_out.shape, w_in.shape)
    grad_mlp_w, grad_win = spread_mlp(pos_x, own0, mate0, 0, shapes, ())
    grad_mlp_w, grad_win = spread_mlp(pos_y, own1, mate1, 1, shapes, (grad_mlp_w, grad_win))
    grad_win, grad_attn_w = spread_attention(pos_x, own2, mate2, grad_win, w_attn_out.shape)
    return (
        block_out, grad_image, small[0:width], grad_win, small[width : width + 64],
        small[width + 64 : width + 128], grad_attn_w, grad_mlp_w,
    )


def solution(mesh):
    tokens = P(("seq", "head"), None)
    return jax.shard_map(
        per_device,
        mesh=mesh,
        in_specs=(tokens, P(), P(), P(), P(), P(), P(), tokens, P("seq", None)),
        out_specs=(tokens, tokens, P(), P(), P(), P(), P(), P()),
        check_vma=False,
    )
```

```python
import functools
import math

import jax
import jax.numpy as jnp
from jax import lax
from jax.experimental import pallas as pl
from jax.experimental.pallas import tpu as pltpu
from jax.sharding import PartitionSpec as P

F32 = jnp.float32
BF16 = jnp.bfloat16
EPS = 1e-06
AXES = ("seq", "head")
VMEM = 32 << 20
BLOCKS = 16
EXCLUDE = 32768.0
SCORE_SCALE = 0.125 * math.log2(math.e)


def dot_nn(a, b):
    return lax.dot_general(a, b, (((1,), (0,)), ((), ())), preferred_element_type=F32)


def dot_nt(a, b):
    return lax.dot_general(a, b, (((1,), (1,)), ((), ())), preferred_element_type=F32)


def dot_tn(a, b):
    return lax.dot_general(a, b, (((0,), (0,)), ((), ())), preferred_element_type=F32)


def row_sums(x):
    ones = jnp.ones((8, x.shape[1]), BF16)
    high = x.astype(BF16)
    low = (x - high.astype(F32)).astype(BF16)
    return dot_nt(ones, high) + dot_nt(ones, low)


def prep_body(ids_ref, image_ref, cot_ref, gain_ref, out_ref):
    tokens, width = image_ref.shape
    step = 64
    for r in range(0, tokens, step):
        x = image_ref[r : r + step, :].astype(F32)
        center = x - jnp.mean(x, axis=-1, keepdims=True)
        spread = jnp.mean(center * center, axis=-1, keepdims=True)
        out_ref[r : r + step, 0:width] = (center * lax.rsqrt(spread + EPS) * gain_ref[...]).astype(BF16)
    out_ref[:, width : 2 * width] = cot_ref[...]
    ids = ids_ref[...]
    image = lax.broadcasted_iota(jnp.int32, (128, tokens), 0) & 63
    marks = jnp.where(image == ids, 1.0, 0.0).astype(F32)
    out_ref[:, 2 * width :] = jnp.transpose(marks).astype(BF16)


def prep(ids, image_in, cotangent, ln_gain):
    tokens, width = image_in.shape
    return pl.pallas_call(
        prep_body,
        out_shape=jax.ShapeDtypeStruct((tokens, 2 * width + 128), BF16),
        cost_estimate=pl.CostEstimate(flops=10 * tokens * width, bytes_accessed=8 * tokens * width, transcendentals=0),
        name="prep",
    )(ids, image_in, cotangent, ln_gain)


def mlp_body(
    pos_ref, normed_ref, cot_ref, win_ref, wout_ref, grads_ref, bo_ref, dn_ref, ln_ref, up_s, dact_s, act_s, dup_s
):
    tokens, width = normed_ref.shape
    sid = pos_ref[1]
    up_s[...] = dot_nn(normed_ref[...], win_ref[...])
    dact_s[...] = dot_nt(cot_ref[...], wout_ref[...])
    step = 32

    def gelu_rows(i, carry):
        rows = pl.ds(pl.multiple_of(i * step, step), step)
        up = up_s[rows, :]
        cdf = 0.5 * (1.0 + lax.erf(up * math.sqrt(0.5)))
        pdf = jnp.exp(-0.5 * up * up) * (1.0 / math.sqrt(2.0 * math.pi))
        act_s[rows, :] = (up * cdf).astype(BF16)
        dup_s[rows, :] = (dact_s[rows, :] * (cdf + up * pdf)).astype(BF16)
        return carry

    lax.fori_loop(0, tokens // step, gelu_rows, 0)
    rows = width // BLOCKS
    part = 384
    first = pl.program_id(0) == 0
    for j in range(0, width, part):
        grad_out = dot_tn(act_s[:, j : j + part], cot_ref[...])
        grad_in = dot_tn(normed_ref[:, j : j + part], dup_s[...])
        ln_terms = row_sums(grad_in * win_ref[j : j + part, :].astype(F32))

        @pl.when(first)
        def _(j=j, ln_terms=ln_terms):
            ln_ref[:, j : j + part] = ln_terms

        @pl.when(jnp.logical_not(first))
        def _(j=j, ln_terms=ln_terms):
            ln_ref[:, j : j + part] += ln_terms

        for i in range(part // rows):
            where = (j // rows + i) ^ sid
            grads_ref[0, where, 0:rows, :] = grad_out[i * rows : (i + 1) * rows].astype(BF16)
            grads_ref[0, where, rows : 2 * rows, :] = grad_in[i * rows : (i + 1) * rows].astype(BF16)
    bo = dot_nn(act_s[...], wout_ref[...])
    dn = dot_nt(dup_s[...], win_ref[...])

    @pl.when(first)
    def _():
        bo_ref[...] = bo
        dn_ref[...] = dn

    @pl.when(jnp.logical_not(first))
    def _():
        bo_ref[...] += bo
        dn_ref[...] += dn


def mlp(pos, packed, w_in, w_mlp_out, part):
    tokens = packed.shape[0]
    width = w_mlp_out.shape[1]
    rows = width // BLOCKS
    first = 3 + 2 * part
    return pl.pallas_call(
        mlp_body,
        out_shape=(
            jax.ShapeDtypeStruct((2, BLOCKS, 2 * rows, width), BF16),
            jax.ShapeDtypeStruct((tokens, width), F32),
            jax.ShapeDtypeStruct((tokens, width), F32),
            jax.ShapeDtypeStruct((8, width), F32),
        ),
        grid_spec=pltpu.PrefetchScalarGridSpec(
            num_scalar_prefetch=1,
            grid=(2,),
            in_specs=[
                pl.BlockSpec((tokens, width), lambda t, pos: (0, 0)),
                pl.BlockSpec((tokens, width), lambda t, pos: (0, 1)),
                pl.BlockSpec((width, width), lambda t, pos: (0, first + t)),
                pl.BlockSpec((width, width), lambda t, pos: (2 * part + t, 0)),
            ],
            out_specs=[
                pl.BlockSpec((1, BLOCKS, 2 * rows, width), lambda t, pos: (t ^ pos[0], 0, 0, 0)),
                pl.BlockSpec((tokens, width), lambda t, pos: (0, 0)),
                pl.BlockSpec((tokens, width), lambda t, pos: (0, 0)),
                pl.BlockSpec((8, width), lambda t, pos: (0, 0)),
            ],
            scratch_shapes=[
                pltpu.VMEM((tokens, width), F32),
                pltpu.VMEM((tokens, width), F32),
                pltpu.VMEM((tokens, width), BF16),
                pltpu.VMEM((tokens, width), BF16),
            ],
        ),
        compiler_params=pltpu.CompilerParams(dimension_semantics=("arbitrary",), vmem_limit_bytes=VMEM),
        cost_estimate=pl.CostEstimate(
            flops=2 * 6 * 2 * tokens * width * width, bytes_accessed=16 * width * width, transcendentals=4 * tokens * width
        ),
        name=f"mlp{part}",
    )(pos, packed, packed, w_in, w_mlp_out)


RUN = 768


def project_body(
    pos_ref, own_ref, mate_ref, wq_ref, wk_ref, wv_ref, wo_ref,
    normed_ref, turned_ref, cot_ref, marks_ref, raw_ref, dout_ref, start_ref, twice_s,
):
    tokens, packed = own_ref.shape
    width = wo_ref.shape[1]
    group = 2 * tokens
    block = 128
    twice_s[0:tokens, :] = own_ref[...]
    twice_s[tokens:group, :] = mate_ref[...]
    twice_s[group : group + block, :] = own_ref[0:block, :]
    marks = twice_s[0:group, 2 * width :]
    held = dot_nn(jnp.ones((8, group), BF16), marks)
    lane = lax.broadcasted_iota(jnp.int32, (8, 128), 1)
    chosen = jnp.where(jnp.logical_and(held == float(RUN), lane < 64), 1.0, 0.0).astype(BF16)
    inside = dot_nt(chosen, marks)
    before = pltpu.roll(inside, 1, 1)
    place = lax.broadcasted_iota(jnp.int32, (8, group), 1).astype(F32)
    opens = jnp.where(jnp.logical_and(inside > 0.5, before < 0.5), place, 0.0)
    start = jnp.sum(opens[0:1, :]).astype(jnp.int32)
    start_ref[0] = start
    high, rest = start // block, start % block
    row = lax.broadcasted_iota(jnp.int32, (block, 2 * block), 0)
    col = lax.broadcasted_iota(jnp.int32, (block, 2 * block), 1)
    shift = jnp.where(col == row + rest, 1.0, 0.0).astype(BF16)
    for i in range(group // block):
        at = pl.multiple_of(((i + high) % (group // block)) * block, block)
        moved = dot_nn(shift, twice_s[pl.ds(at, 2 * block), :]).astype(BF16)
        rows = slice(i * block, (i + 1) * block)
        normed_ref[rows, :] = moved[:, 0:width]
        cot_ref[rows, :] = moved[:, width : 2 * width]
        marks_ref[rows, :] = moved[:, 2 * width :]
    for n, w_ref in enumerate((wq_ref, wk_ref, wv_ref)):
        raw_ref[n, :, :] = dot_nn(normed_ref[...], w_ref[...]).astype(BF16)
    dout_ref[...] = dot_nt(cot_ref[...], wo_ref[...]).astype(BF16)
    for j in range(0, width, 128):
        turned_ref[j : j + 128, :] = jnp.transpose(normed_ref[:, j : j + 128].astype(F32)).astype(BF16)


def project(pos, own, mate, w_in, w_attn_out):
    tokens, packed = own.shape
    width = w_attn_out.shape[1]
    group = 2 * tokens
    part = width // 2

    def whole(shape):
        return pl.BlockSpec(shape, lambda i, pos: (0,) * len(shape))

    outs = [(group, width), (width, group), (group, width), (group, 128), (3, group, part), (group, part)]
    return pl.pallas_call(
        project_body,
        out_shape=tuple(jax.ShapeDtypeStruct(s, BF16) for s in outs) + (jax.ShapeDtypeStruct((1,), jnp.int32),),
        grid_spec=pltpu.PrefetchScalarGridSpec(
            num_scalar_prefetch=1,
            grid=(1,),
            in_specs=[
                whole(own.shape),
                whole(own.shape),
                pl.BlockSpec((width, part), lambda i, pos: (0, pos[0])),
                pl.BlockSpec((width, part), lambda i, pos: (0, 2 + pos[0])),
                pl.BlockSpec((width, part), lambda i, pos: (0, 4 + pos[0])),
                pl.BlockSpec((part, width), lambda i, pos: (pos[0], 0)),
            ],
            out_specs=[whole(s) for s in outs] + [pl.BlockSpec(memory_space=pltpu.SMEM)],
            scratch_shapes=[pltpu.VMEM((group + 128, packed), BF16)],
        ),
        cost_estimate=pl.CostEstimate(
            flops=2 * group * width * 4 * part, bytes_accessed=14 * group * width, transcendentals=0
        ),
        compiler_params=pltpu.CompilerParams(vmem_limit_bytes=VMEM),
        name="project",
    )(pos, own, mate, w_in, w_in, w_in, w_attn_out)


def split_dot(x, ones):
    high = x.astype(BF16)
    low = (x - high.astype(F32)).astype(BF16)
    return dot_nn(high, ones) + dot_nn(low, ones)


def attend_body(
    pos_ref, q_ref, k_ref, v_ref, dout_ref, marks_ref, turned_ref, cot_ref, gq_ref, gk_ref, wq_ref, wk_ref, wv_ref,
    before_ref, lns_ref, gains_in_ref, grads_ref, dproj_ref, att_ref, gains_ref, ln_ref,
    q_s, k_s, v_s, unit_s, rstd_s, e_s, ds_s, g_s, dq_s, dk_s, dv_s,
):
    group = q_ref.shape[1]
    width = cot_ref.shape[1]
    size = 64
    sid = pos_ref[1]
    step = 256

    def lanes(rows):
        return lax.broadcasted_iota(jnp.int32, (rows, 128), 1)

    same = lax.broadcasted_iota(jnp.int32, (128, 128), 0) // size == lax.broadcasted_iota(jnp.int32, (128, 128), 1) // size
    ones = jnp.where(same, 1.0, 0.0).astype(BF16)

    for r in range(0, group, step):
        rows = slice(r, r + step)
        low = lanes(step) < size
        marks = marks_ref[rows, :].astype(F32)
        away = (marks - 1.0) * EXCLUDE
        v = v_ref[0, rows, :].astype(F32)
        scaled = []
        for n, (raw_ref, gain_ref) in enumerate(((q_ref, gq_ref), (k_ref, gk_ref))):
            raw = raw_ref[0, rows, :]
            center = raw.astype(F32) - dot_nn(raw, ones) * (1.0 / size)
            rstd = lax.rsqrt(split_dot(center * center, ones) * (1.0 / size) + EPS)
            unit = center * rstd
            unit_s[n, rows, :] = unit
            rstd_s[n, rows, :] = rstd
            scaled.append(unit * gain_ref[...])
        for h in range(2):
            mine = low if h == 0 else jnp.logical_not(low)
            q_s[h, rows, :] = jnp.where(mine, scaled[0], marks).astype(BF16)
            k_s[h, rows, :] = jnp.where(mine, scaled[1], away).astype(BF16)
            v_s[h, rows, :] = jnp.where(mine, v, 1.0).astype(BF16)

    block = 256
    for h in range(2):
        for first, count in ((0, RUN), (RUN, group - RUN)):
            span = slice(first, first + count)
            for i in range(0, count, block):
                rows = slice(first + i, first + i + block)
                scores = dot_nt(q_s[h, rows, :], k_s[h, span, :])
                e_s[h, i : i + block, 0:count] = jnp.exp2(scores * SCORE_SCALE).astype(BF16)
            for i in range(0, count, block):
                rows = slice(first + i, first + i + block)
                lane = lanes(block)
                mine = (lane < size) if h == 0 else (lane >= size)
                spare = size if h == 0 else 0
                outs = dot_nn(e_s[h, i : i + block, 0:count], v_s[h, span, :])
                inverse = 1.0 / pltpu.roll(outs, size, 1)
                attended = outs * inverse
                grad_low = (dout_ref[rows, :].astype(F32) * inverse).astype(BF16).astype(F32)
                centre = split_dot(jnp.where(mine, grad_low * attended, 0.0), jnp.ones((128, 128), BF16))
                centre_high = centre.astype(BF16).astype(F32)
                extra = jnp.where(lane == spare, -centre_high, jnp.where(lane == spare + 1, centre_high - centre, 0.0))
                grad_ext = jnp.where(mine, grad_low, extra).astype(BF16)
                g_s[h, rows, :] = grad_ext
                if h == 0:
                    att_ref[rows, :] = attended.astype(BF16)
                else:
                    att_ref[rows, :] = jnp.where(mine, attended, att_ref[rows, :].astype(F32)).astype(BF16)
                d_probs = dot_nt(grad_ext, v_s[h, span, :])
                ds_s[h, i : i + block, 0:count] = (e_s[h, i : i + block, 0:count].astype(F32) * d_probs).astype(BF16)
            dq_s[h, span, :] = dot_nn(ds_s[h, 0:count, 0:count], k_s[h, span, :])
            dk_s[h, span, :] = dot_tn(ds_s[h, 0:count, 0:count], q_s[h, span, :])
            dv_s[h, span, :] = dot_tn(e_s[h, 0:count, 0:count], g_s[h, span, :])

    for r in range(0, group, step):
        rows = slice(r, r + step)
        low = lanes(step) < size
        for n, (grad_s, gain_ref) in enumerate(((dq_s, gq_ref), (dk_s, gk_ref))):
            unit, rstd = unit_s[n, rows, :], rstd_s[n, rows, :]
            grad = jnp.where(low, grad_s[0, rows, :], grad_s[1, rows, :]) * 0.125
            part = jnp.sum((grad * unit).reshape(step // 8, 8, 128), axis=0)
            if r == 0:
                gains_ref[8 * n : 8 * (n + 1), :] = gains_in_ref[8 * n : 8 * (n + 1), :] + part
            else:
                gains_ref[8 * n : 8 * (n + 1), :] += part
            grad = grad * gain_ref[...]
            mean = split_dot(grad, ones) * (1.0 / size)
            slope = split_dot(grad * unit, ones) * (1.0 / size)
            dproj_ref[rows, 128 * n : 128 * (n + 1)] = (rstd * (grad - mean - unit * slope)).astype(BF16)
        dproj_ref[rows, 256:384] = jnp.where(low, dv_s[0, rows, :], dv_s[1, rows, :]).astype(BF16)

    rows = width // BLOCKS
    part = 384
    for j in range(0, width, part):
        grad_in = dot_nn(turned_ref[j : j + part, :], dproj_ref[...])
        terms = lns_ref[:, j : j + part]
        for n, w_ref in enumerate((wq_ref, wk_ref, wv_ref)):
            terms += row_sums(grad_in[:, 128 * n : 128 * (n + 1)] * w_ref[j : j + part, :].astype(F32))
        ln_ref[:, j : j + part] = terms
        for i in range(part // rows):
            grads_ref[(j // rows + i) ^ sid, 0:rows, :] = grad_in[i * rows : (i + 1) * rows].astype(BF16)
    grad_out = dot_tn(att_ref[...], cot_ref[...])
    few = 128 // BLOCKS
    for i in range(BLOCKS):
        piece = grad_out[i * few : (i + 1) * few]
        piece = jnp.concatenate([piece[:, :384], piece[:, 384:]], axis=0)
        grads_ref[i ^ sid, rows : rows + 2 * few, :] = piece.astype(BF16)
    rows += 2 * few
    if grads_ref.shape[1] > rows:
        gains = jnp.sum(gains_ref[...].reshape(2, 8, 128), axis=1)
        gains = gains + pltpu.roll(gains, size, 1)
        gains = jnp.where(lanes(1) < size, gains[0:1], gains[1:2])
        small = [ln_ref[0:1, 0:384], ln_ref[0:1, 384:768], jnp.concatenate([gains, jnp.zeros((1, 256), F32)], axis=1)]
        small = jnp.concatenate(small + [jnp.zeros((5, 384), F32)], axis=0)
        for i in range(BLOCKS):
            grads_ref[i ^ sid, rows : rows + 8, :] = (small if i == 0 else jnp.zeros_like(small)).astype(BF16)


def attend(pos, pair, projected, gain_q, gain_k, w_in, before, lns, gains):
    normed, turned, cot, marks, raw, dout, _ = projected
    group, width = normed.shape
    last = pair == 2
    rows = width // BLOCKS + 16 + 8 * last
    cols = 384 if last else 768
    alias = {13: 0} if pair == 1 else {}
    before_spec = pl.BlockSpec(memory_space=pl.ANY)

    def whole(shape):
        return pl.BlockSpec(shape, lambda i, pos: (0,) * len(shape))

    raw_specs = [pl.BlockSpec((1, group, 128), lambda i, pos, n=n: (n, 0, pair)) for n in range(3)]
    return pl.pallas_call(
        attend_body,
        out_shape=(
            jax.ShapeDtypeStruct((BLOCKS, rows, cols), BF16),
            jax.ShapeDtypeStruct((group, 384), BF16),
            jax.ShapeDtypeStruct((group, 128), BF16),
            jax.ShapeDtypeStruct((16, 128), F32),
            jax.ShapeDtypeStruct((8, width), F32),
        ),
        grid_spec=pltpu.PrefetchScalarGridSpec(
            num_scalar_prefetch=1,
            grid=(1,),
            in_specs=raw_specs
            + [
                pl.BlockSpec((group, 128), lambda i, pos: (0, pair)),
                whole(marks.shape),
                whole(turned.shape),
                whole(cot.shape),
                whole((1, 128)),
                whole((1, 128)),
            ]
            + [pl.BlockSpec((width, 128), lambda i, pos, n=n: (0, 6 * n + 3 * pos[0] + pair)) for n in range(3)]
            + [before_spec, whole((8, width)), whole((16, 128))],
            out_specs=[
                pl.BlockSpec((BLOCKS, rows, 384), lambda i, pos: (0, 0, 1 if pair == 1 else 0)),
                whole((group, 384)),
                whole((group, 128)),
                whole((16, 128)),
                whole((8, width)),
            ],
            scratch_shapes=[
                pltpu.VMEM((2, group, 128), BF16),
                pltpu.VMEM((2, group, 128), BF16),
                pltpu.VMEM((2, group, 128), BF16),
                pltpu.VMEM((2, group, 128), F32),
                pltpu.VMEM((2, group, 128), F32),
                pltpu.VMEM((2, RUN, RUN), BF16),
                pltpu.VMEM((2, RUN, RUN), BF16),
                pltpu.VMEM((2, group, 128), BF16),
                pltpu.VMEM((2, group, 128), F32),
                pltpu.VMEM((2, group, 128), F32),
                pltpu.VMEM((2, group, 128), F32),
            ],
        ),
        input_output_aliases=alias,
        compiler_params=pltpu.CompilerParams(vmem_limit_bytes=VMEM),
        cost_estimate=pl.CostEstimate(
            flops=8 * 10**9, bytes_accessed=6 * group * width, transcendentals=2 * RUN * RUN
        ),
        name=f"attend{pair}",
    )(pos, raw, raw, raw, dout, marks, turned, cot, gain_q, gain_k, w_in, w_in, w_in, before, lns, gains)


def combine_body(pos_ref, start_ref, *refs):
    weights, dprojs, atts = refs[0:12], refs[12:15], refs[15:18]
    part_ref, both_s = refs[18:]
    group, width = atts[0].shape[0], weights[3].shape[1]
    bo = sum(dot_nn(atts[p][...], weights[4 * p + 3][...]) for p in range(3))
    both_s[0:group, 0:width] = bo.astype(BF16)
    dn = None
    for p in range(3):
        for n in range(3):
            term = dot_nt(dprojs[p][:, 128 * n : 128 * (n + 1)], weights[4 * p + n][...])
            dn = term if dn is None else dn + term
    both_s[0:group, width : 2 * width] = dn.astype(BF16)
    block = 128
    both_s[group : group + block, :] = both_s[0:block, :]
    back = group - start_ref[0]
    high, rest = back // block, back % block
    row = lax.broadcasted_iota(jnp.int32, (block, 2 * block), 0)
    col = lax.broadcasted_iota(jnp.int32, (block, 2 * block), 1)
    shift = jnp.where(col == row + rest, 1.0, 0.0).astype(BF16)
    half = group // (2 * block)
    for i in range(group // block):
        at = pl.multiple_of(((i + high) % (group // block)) * block, block)
        moved = dot_nn(shift, both_s[pl.ds(at, 2 * block), :]).astype(BF16)
        part_ref[i // half, (i % half) * block : (i % half + 1) * block, :] = moved


def combine(pos, start, w_in, w_attn_out, dprojs, atts):
    group, width = atts[0].shape[0], w_attn_out.shape[1]

    def whole(shape):
        return pl.BlockSpec(shape, lambda i, pos, start: (0,) * len(shape))

    weights, specs = [], []
    for p in range(3):
        for n in range(3):
            weights.append(w_in)
            specs.append(pl.BlockSpec((width, 128), lambda i, pos, start, p=p, n=n: (0, 6 * n + 3 * pos[0] + p)))
        weights.append(w_attn_out)
        specs.append(pl.BlockSpec((128, width), lambda i, pos, start, p=p: (3 * pos[0] + p, 0)))
    out = (2, group // 2, 2 * width)
    return pl.pallas_call(
        combine_body,
        out_shape=jax.ShapeDtypeStruct(out, BF16),
        grid_spec=pltpu.PrefetchScalarGridSpec(
            num_scalar_prefetch=2,
            grid=(1,),
            in_specs=specs + [whole((group, 384))] * 3 + [whole((group, 128))] * 3,
            out_specs=whole(out),
            scratch_shapes=[pltpu.VMEM((group + 128, 2 * width), BF16)],
        ),
        cost_estimate=pl.CostEstimate(flops=5 * 10**9, bytes_accessed=12 * group * width, transcendentals=0),
        compiler_params=pltpu.CompilerParams(vmem_limit_bytes=VMEM),
        name="combine",
    )(pos, start, *weights, *dprojs, *atts)


def finish_body(
    pos_ref, image_ref, cot_ref, gain_ref, bo_ref, dn_ref, bo2_ref, dn2_ref, joined_ref, got_ref, out_ref, grad_ref
):
    tokens, width = image_ref.shape
    step = 64
    stays = pos_ref[0] == pos_ref[2]

    def put(source):
        for r in range(0, tokens, step):
            rows = slice(r, r + step)
            x = image_ref[rows, :].astype(F32)
            here = source[rows, :].astype(F32)
            out_ref[rows, :] = (x + (bo_ref[rows, :] + bo2_ref[rows, :] + here[:, 0:width])).astype(BF16)
            center = x - jnp.mean(x, axis=-1, keepdims=True)
            rstd = lax.rsqrt(jnp.mean(center * center, axis=-1, keepdims=True) + EPS)
            scaled = center * rstd
            grad = dn_ref[rows, :] + dn2_ref[rows, :] + here[:, width : 2 * width]
            grad = grad * gain_ref[...]
            mean = jnp.mean(grad, axis=-1, keepdims=True)
            slope = jnp.mean(grad * scaled, axis=-1, keepdims=True)
            grad_ref[rows, :] = cot_ref[rows, :].astype(F32) + rstd * (grad - mean - scaled * slope)

    pl.when(stays)(lambda: put(joined_ref))
    pl.when(jnp.logical_not(stays))(lambda: put(got_ref))


def finish(pos, image_in, cotangent, ln_gain, bo, dn, bo2, dn2, joined, got):
    tokens, width = image_in.shape
    vmem = pl.BlockSpec(memory_space=pltpu.VMEM)
    return pl.pallas_call(
        finish_body,
        out_shape=(jax.ShapeDtypeStruct((tokens, width), BF16), jax.ShapeDtypeStruct((tokens, width), F32)),
        in_specs=[pl.BlockSpec(memory_space=pltpu.SMEM)] + [vmem] * 9,
        out_specs=(vmem, vmem),
        compiler_params=pltpu.CompilerParams(vmem_limit_bytes=VMEM),
        cost_estimate=pl.CostEstimate(flops=30 * tokens * width, bytes_accessed=30 * tokens * width, transcendentals=0),
        name="finish",
    )(pos, image_in, cotangent, ln_gain, bo, dn, bo2, dn2, joined, got)


def exchange(value, mask):
    count = lax.axis_size(AXES)
    return lax.ppermute(value, AXES, [(i, i ^ mask) for i in range(count)])


def add_low(left, right):
    return (left.astype(F32) + right.astype(F32)).astype(BF16)


def reduce_scatter(chunk, masks, rest):
    for mask in masks:
        half = chunk.shape[0] // 2
        chunk = add_low(chunk[:half], exchange(chunk[half:], mask))
    for mask in rest:
        chunk = add_low(chunk, exchange(chunk, mask))
    return chunk


def all_gather(chunk, masks):
    for mask in reversed(masks):
        chunk = jnp.concatenate([chunk, exchange(chunk, mask)], axis=0)
    return chunk


def spread_mlp_body(pos_ref, own_ref, mate_ref, *refs):
    out_ref, in_ref = refs[-2:]
    sid = pos_ref[1]
    rows = own_ref.shape[1] // 2
    side, quarter = pl.program_id(0), pl.program_id(1)

    def put(source):
        for i in range(4):
            at = (4 * quarter + i) ^ sid
            out_ref[i * rows : (i + 1) * rows, :] = source[at, 0:rows, :].astype(F32)
            in_ref[i * rows : (i + 1) * rows, :] = source[at, rows : 2 * rows, :].astype(F32)

    pl.when(side == 0)(lambda: put(own_ref))
    pl.when(side == 1)(lambda: put(mate_ref))


def spread_mlp(pos, own, mate, part, shapes, before):
    blocks, rows2, width = own.shape
    whole = pl.BlockSpec(own.shape, lambda r, g, pos: (0, 0, 0))
    return pl.pallas_call(
        spread_mlp_body,
        out_shape=tuple(jax.ShapeDtypeStruct(s, F32) for s in shapes),
        grid_spec=pltpu.PrefetchScalarGridSpec(
            num_scalar_prefetch=1,
            grid=(2, 4),
            in_specs=[whole, whole] + [pl.BlockSpec(memory_space=pl.ANY)] * len(before),
            out_specs=[
                pl.BlockSpec((width // 4, width), lambda r, g, pos: (4 * (2 * part + (r ^ pos[0])) + g, 0)),
                pl.BlockSpec((width // 4, width), lambda r, g, pos: (g, 3 + 2 * part + (r ^ pos[0]))),
            ],
        ),
        input_output_aliases={3 + i: i for i in range(len(before))},
        compiler_params=pltpu.CompilerParams(dimension_semantics=("arbitrary", "arbitrary"), vmem_limit_bytes=VMEM),
        cost_estimate=pl.CostEstimate(flops=0, bytes_accessed=24 * width * width, transcendentals=0),
        name=f"spread_mlp{part}",
    )(pos, own, mate, *before)


def spread_attention_body(pos_ref, own_ref, mate_ref, *refs):
    in_ref, out_ref = refs[-3:-1] if own_ref.shape[1] > 64 else refs[-2:]
    sid = pos_ref[1]
    blocks = own_ref.shape[0]
    rows = 48
    side, kind = pl.program_id(0), pl.program_id(2)

    def put(source):
        from_col = pl.ds(pl.multiple_of(128 * kind, 128), 128)
        for i in range(blocks):
            in_ref[i * rows : (i + 1) * rows, :] = source[i ^ sid, 0:rows, from_col].astype(F32)

        @pl.when(kind == 0)
        def _():
            for i in range(blocks):
                piece = source[i ^ sid, rows : rows + 16, :].astype(F32)
                out_ref[8 * i : 8 * (i + 1), 0:384] = piece[0:8]
                out_ref[8 * i : 8 * (i + 1), 384:768] = piece[8:16]

    pl.when(side == 0)(lambda: put(own_ref))
    pl.when(side == 1)(lambda: put(mate_ref))
    if own_ref.shape[1] > 64:
        refs[-1][...] = own_ref[sid, 64:72, :].astype(F32) + mate_ref[sid, 64:72, :].astype(F32)


def spread_attention(pos, own, mate, pairs, shapes, before):
    rows = own.shape[1]
    width = shapes[1][0]
    base = pairs[0]
    block = pl.BlockSpec((BLOCKS, rows, 384), lambda r, p, k, pos: (0, 0, p))
    out_shape = [jax.ShapeDtypeStruct(s, F32) for s in shapes]
    out_specs = [
        pl.BlockSpec((width, 128), lambda r, p, k, pos: (0, 6 * k + 3 * (r ^ pos[0]) + base + p)),
        pl.BlockSpec((128, width), lambda r, p, k, pos: (3 * (r ^ pos[0]) + base + p, 0)),
    ]
    if rows > 64:
        out_shape.append(jax.ShapeDtypeStruct((8, 384), F32))
        out_specs.append(pl.BlockSpec((8, 384), lambda r, p, k, pos: (0, 0)))
    return pl.pallas_call(
        spread_attention_body,
        out_shape=tuple(out_shape),
        grid_spec=pltpu.PrefetchScalarGridSpec(
            num_scalar_prefetch=1,
            grid=(2, len(pairs), 3),
            in_specs=[block, block] + [pl.BlockSpec(memory_space=pl.ANY)] * len(before),
            out_specs=out_specs,
        ),
        input_output_aliases={3 + i: i for i in range(len(before))},
        compiler_params=pltpu.CompilerParams(
            dimension_semantics=("arbitrary",) * 3, vmem_limit_bytes=VMEM
        ),
        cost_estimate=pl.CostEstimate(flops=0, bytes_accessed=16 * width * 384 * len(pairs), transcendentals=0),
        name=f"spread_attention{base}",
    )(pos, own, mate, *before)


def per_device(image_in, ln_gain, w_in, q_gain, k_gain, w_attn_out, w_mlp_out, cotangent, image_ids):
    tokens, width = image_in.shape
    count = lax.axis_size(AXES)
    index = lax.axis_index(AXES)
    side = index & 1
    core = (index >> 1) & 1
    others = [1 << k for k in range(2, count.bit_length() - 1)]
    masks_x = [1] + others[:3]
    masks_y = [others[0], 1] + others[1:3]
    rest = others[3:]
    crossing = [(i, i ^ 3) for i in range(count) if i & 3 in (1, 2)]

    def place(masks):
        sid = jnp.int32(0)
        for mask in masks:
            sid = 2 * sid + ((index & mask) != 0).astype(jnp.int32)
        return jnp.stack([core, sid, side])

    pos_x, pos_y = place(masks_x), place(masks_y)
    gain_row = ln_gain.reshape(1, width)
    gain_q = jnp.concatenate([q_gain, q_gain]).reshape(1, 128)
    gain_k = jnp.concatenate([k_gain, k_gain]).reshape(1, 128)
    ids = lax.dynamic_slice(image_ids, (0, side * tokens), (1, tokens))
    packed = prep(ids, image_in, cotangent, gain_row)
    crossed = lax.ppermute(packed, AXES, crossing)
    grads0, bo0, dn0, ln0 = mlp(pos_y, packed, w_in, w_mlp_out, 0)
    swapped = jnp.where(core == side, packed, crossed)
    mate = exchange(swapped, 2)
    grads1, bo1, dn1, ln1 = mlp(pos_x, packed, w_in, w_mlp_out, 1)

    def gather(chunk, masks):
        own = all_gather(reduce_scatter(chunk, masks, rest), masks)
        return own, exchange(own, 2)

    own0, mate0 = gather(add_low(grads0[0], exchange(grads0[1], 2)), masks_y)
    own1, mate1 = gather(add_low(grads1[0], exchange(grads1[1], 2)), masks_x)

    projected = project(pos_x, swapped, mate, w_in, w_attn_out)
    empty = jnp.zeros((8, 128), BF16)
    first = attend(pos_y, 0, projected, gain_q, gain_k, w_in, empty, ln0 + ln1, jnp.zeros((16, 128), F32))
    second = attend(pos_y, 1, projected, gain_q, gain_k, w_in, first[0], first[4], first[3])
    third = attend(pos_x, 2, projected, gain_q, gain_k, w_in, empty, second[4], second[3])
    own2, mate2 = gather(second[0], masks_y)
    own3, mate3 = gather(third[0], masks_x)
    pieces = (first, second, third)
    parts = combine(pos_x, projected[6], w_in, w_attn_out, [p[1] for p in pieces], [p[2] for p in pieces])
    joined = add_low(parts[0], exchange(parts[1], 2))
    got = lax.ppermute(joined, AXES, crossing)
    block_out, grad_image = finish(pos_x, image_in, cotangent, gain_row, bo0, dn0, bo1, dn1, joined, got)
    shapes = (w_mlp_out.shape, w_in.shape)
    grad_mlp_w, grad_win = spread_mlp(pos_y, own0, mate0, 0, shapes, ())
    grad_mlp_w, grad_win = spread_mlp(pos_x, own1, mate1, 1, shapes, (grad_mlp_w, grad_win))
    shapes = (w_in.shape, w_attn_out.shape)
    grad_win, grad_attn_w = spread_attention(pos_y, own2, mate2, (0, 1), shapes, (grad_win,))
    grad_win, grad_attn_w, small = spread_attention(pos_x, own3, mate3, (2,), shapes, (grad_win, grad_attn_w))
    small = small.reshape(-1)
    return (
        block_out, grad_image, small[0:width] / ln_gain, grad_win, small[width : width + 64],
        small[width + 64 : width + 128], grad_attn_w, grad_mlp_w,
    )


def solution(mesh):
    tokens = P(("seq", "head"), None)
    return jax.shard_map(
        per_device,
        mesh=mesh,
        in_specs=(tokens, P(), P(), P(), P(), P(), P(), tokens, P("seq", None)),
        out_specs=(tokens, tokens, P(), P(), P(), P(), P(), P()),
        check_vma=False,
    )
```

```python
import functools
import math

import jax
import jax.numpy as jnp
from jax import lax
from jax.experimental import pallas as pl
from jax.experimental.pallas import tpu as pltpu
from jax.sharding import PartitionSpec as P

F32 = jnp.float32
BF16 = jnp.bfloat16
EPS = 1e-06
AXES = ("seq", "head")
VMEM = 32 << 20
BLOCKS = 16
EXCLUDE = 32768.0
SHORT = pl.CostEstimate(flops=1, bytes_accessed=1, transcendentals=0)
SCORE_SCALE = 0.125 * math.log2(math.e)


def dot_nn(a, b):
    return lax.dot_general(a, b, (((1,), (0,)), ((), ())), preferred_element_type=F32)


def dot_nt(a, b):
    return lax.dot_general(a, b, (((1,), (1,)), ((), ())), preferred_element_type=F32)


def dot_tn(a, b):
    return lax.dot_general(a, b, (((0,), (0,)), ((), ())), preferred_element_type=F32)


def row_sums(x):
    ones = jnp.ones((8, x.shape[1]), BF16)
    high = x.astype(BF16)
    low = (x - high.astype(F32)).astype(BF16)
    return dot_nt(ones, high) + dot_nt(ones, low)


def prep_body(ids_ref, image_ref, cot_ref, gain_ref, out_ref):
    tokens, width = image_ref.shape
    step = 64
    for r in range(0, tokens, step):
        x = image_ref[r : r + step, :].astype(F32)
        center = x - jnp.mean(x, axis=-1, keepdims=True)
        spread = jnp.mean(center * center, axis=-1, keepdims=True)
        out_ref[r : r + step, 0:width] = (center * lax.rsqrt(spread + EPS) * gain_ref[...]).astype(BF16)
    out_ref[:, width : 2 * width] = cot_ref[...]
    ids = ids_ref[...]
    image = lax.broadcasted_iota(jnp.int32, (128, tokens), 0) & 63
    marks = jnp.where(image == ids, 1.0, 0.0).astype(F32)
    out_ref[:, 2 * width :] = jnp.transpose(marks).astype(BF16)


def prep(ids, image_in, cotangent, ln_gain):
    tokens, width = image_in.shape
    return pl.pallas_call(
        prep_body,
        out_shape=jax.ShapeDtypeStruct((tokens, 2 * width + 128), BF16),
        cost_estimate=SHORT,
        name="prep",
    )(ids, image_in, cotangent, ln_gain)


def mlp_body(
    pos_ref, own_ref, mate_ref, win_ref, wout_ref, *refs,
):
    before = refs[:-11]
    keep_ref, send_ref, here_ref, there_ref, ln_ref, normed_s, cot_s, up_s, dact_s, act_s, dup_s = refs[-11:]
    tokens = own_ref.shape[0]
    width = wout_ref.shape[1]
    sid = pos_ref[1]
    for i, ref in enumerate((own_ref, mate_ref)):
        normed_s[i * tokens : (i + 1) * tokens, :] = ref[:, 0:width]
        cot_s[i * tokens : (i + 1) * tokens, :] = ref[:, width : 2 * width]
    up_s[...] = dot_nn(normed_s[...], win_ref[...])
    dact_s[...] = dot_nt(cot_s[...], wout_ref[...])
    step = 32

    def gelu_rows(i, carry):
        rows = pl.ds(pl.multiple_of(i * step, step), step)
        up = up_s[rows, :]
        cdf = 0.5 * (1.0 + lax.erf(up * math.sqrt(0.5)))
        pdf = jnp.exp(-0.5 * up * up) * (1.0 / math.sqrt(2.0 * math.pi))
        act_s[rows, :] = (up * cdf).astype(BF16)
        dup_s[rows, :] = (dact_s[rows, :] * (cdf + up * pdf)).astype(BF16)
        return carry

    lax.fori_loop(0, 2 * tokens // step, gelu_rows, 0)
    rows = width // BLOCKS
    part = width // 2
    for other, ref in enumerate((keep_ref, send_ref)):
        cols = pl.ds(pl.multiple_of((sid // (BLOCKS // 2) ^ other) * part, part), part)
        grad_out = dot_tn(act_s[:, cols], cot_s[...])
        grad_in = dot_tn(normed_s[:, cols], dup_s[...])
        ln_ref[:, cols] = row_sums(grad_in * win_ref[cols, :].astype(F32))
        for i in range(BLOCKS // 2):
            where = i ^ (sid % (BLOCKS // 2))
            ref[where, 0:rows, :] = grad_out[i * rows : (i + 1) * rows].astype(BF16)
            ref[where, rows : 2 * rows, :] = grad_in[i * rows : (i + 1) * rows].astype(BF16)
    for side in range(2):
        cols = slice(side * width, (side + 1) * width)
        here = dot_nt(dup_s[0:tokens, :], win_ref[...]) if side else dot_nn(act_s[0:tokens, :], wout_ref[...])
        there = dot_nt(dup_s[tokens:, :], win_ref[...]) if side else dot_nn(act_s[tokens:, :], wout_ref[...])
        if before:
            here += before[0][:, cols]
            there += before[1][:, cols].astype(F32)
        here_ref[:, cols] = here
        there_ref[:, cols] = there.astype(BF16)


def mlp(pos, own, mate, w_in, w_mlp_out, part, before):
    tokens = own.shape[0]
    width = w_mlp_out.shape[1]
    rows = width // BLOCKS

    def whole(shape):
        return pl.BlockSpec(shape, lambda i, pos: (0,) * len(shape))

    half = (BLOCKS // 2, 2 * rows, width)
    outs = [half, half, (tokens, 2 * width), (tokens, 2 * width), (8, width)]
    return pl.pallas_call(
        mlp_body,
        out_shape=tuple(jax.ShapeDtypeStruct(s, t) for s, t in zip(outs, (BF16, BF16, F32, BF16, F32))),
        grid_spec=pltpu.PrefetchScalarGridSpec(
            num_scalar_prefetch=1,
            grid=(1,),
            in_specs=[
                whole(own.shape),
                whole(own.shape),
                pl.BlockSpec((width, width), lambda i, pos: (0, 3 + 2 * pos[0] + part)),
                pl.BlockSpec((width, width), lambda i, pos: (2 * pos[0] + part, 0)),
            ]
            + [whole(x.shape) for x in before],
            out_specs=[whole(s) for s in outs],
            scratch_shapes=[pltpu.VMEM((2 * tokens, width), t) for t in (BF16, BF16, F32, F32, BF16, BF16)],
        ),
        compiler_params=pltpu.CompilerParams(dimension_semantics=("arbitrary",), vmem_limit_bytes=54 << 20),
        cost_estimate=SHORT,
        name=f"mlp{part}",
    )(pos, own, mate, w_in, w_mlp_out, *before)


RUN = 768


def project_body(
    pos_ref, own_ref, mate_ref, wq_ref, wk_ref, wv_ref, wo_ref,
    normed_ref, turned_ref, cot_ref, marks_ref, raw_ref, dout_ref, start_ref, twice_s,
):
    tokens, packed = own_ref.shape
    width = wo_ref.shape[1]
    group = 2 * tokens
    block = 128
    twice_s[0:tokens, :] = own_ref[...]
    twice_s[tokens:group, :] = mate_ref[...]
    twice_s[group : group + block, :] = own_ref[0:block, :]
    marks = twice_s[0:group, 2 * width :]
    held = dot_nn(jnp.ones((8, group), BF16), marks)
    lane = lax.broadcasted_iota(jnp.int32, (8, 128), 1)
    chosen = jnp.where(jnp.logical_and(held == float(RUN), lane < 64), 1.0, 0.0).astype(BF16)
    inside = dot_nt(chosen, marks)
    before = pltpu.roll(inside, 1, 1)
    place = lax.broadcasted_iota(jnp.int32, (8, group), 1).astype(F32)
    opens = jnp.where(jnp.logical_and(inside > 0.5, before < 0.5), place, 0.0)
    start = jnp.sum(opens[0:1, :]).astype(jnp.int32)
    start_ref[0] = start
    high, rest = start // block, start % block
    row = lax.broadcasted_iota(jnp.int32, (block, 2 * block), 0)
    col = lax.broadcasted_iota(jnp.int32, (block, 2 * block), 1)
    shift = jnp.where(col == row + rest, 1.0, 0.0).astype(BF16)
    for i in range(group // block):
        at = pl.multiple_of(((i + high) % (group // block)) * block, block)
        moved = dot_nn(shift, twice_s[pl.ds(at, 2 * block), :]).astype(BF16)
        rows = slice(i * block, (i + 1) * block)
        normed_ref[rows, :] = moved[:, 0:width]
        cot_ref[rows, :] = moved[:, width : 2 * width]
        marks_ref[rows, :] = moved[:, 2 * width :]
    for n, w_ref in enumerate((wq_ref, wk_ref, wv_ref)):
        raw_ref[n, :, :] = dot_nn(normed_ref[...], w_ref[...]).astype(BF16)
    dout_ref[...] = dot_nt(cot_ref[...], wo_ref[...]).astype(BF16)
    for j in range(0, width, 128):
        turned_ref[j : j + 128, :] = jnp.transpose(normed_ref[:, j : j + 128].astype(F32)).astype(BF16)


def project(pos, own, mate, w_in, w_attn_out):
    tokens, packed = own.shape
    width = w_attn_out.shape[1]
    group = 2 * tokens
    part = width // 2

    def whole(shape):
        return pl.BlockSpec(shape, lambda i, pos: (0,) * len(shape))

    outs = [(group, width), (width, group), (group, width), (group, 128), (3, group, part), (group, part)]
    return pl.pallas_call(
        project_body,
        out_shape=tuple(jax.ShapeDtypeStruct(s, BF16) for s in outs) + (jax.ShapeDtypeStruct((1,), jnp.int32),),
        grid_spec=pltpu.PrefetchScalarGridSpec(
            num_scalar_prefetch=1,
            grid=(1,),
            in_specs=[
                whole(own.shape),
                whole(own.shape),
                pl.BlockSpec((width, part), lambda i, pos: (0, pos[0])),
                pl.BlockSpec((width, part), lambda i, pos: (0, 2 + pos[0])),
                pl.BlockSpec((width, part), lambda i, pos: (0, 4 + pos[0])),
                pl.BlockSpec((part, width), lambda i, pos: (pos[0], 0)),
            ],
            out_specs=[whole(s) for s in outs] + [pl.BlockSpec(memory_space=pltpu.SMEM)],
            scratch_shapes=[pltpu.VMEM((group + 128, packed), BF16)],
        ),
        cost_estimate=SHORT,
        compiler_params=pltpu.CompilerParams(vmem_limit_bytes=VMEM),
        name="project",
    )(pos, own, mate, w_in, w_in, w_in, w_attn_out)


def split_dot(x, ones):
    high = x.astype(BF16)
    low = (x - high.astype(F32)).astype(BF16)
    return dot_nn(high, ones) + dot_nn(low, ones)


def attend_body(
    pos_ref, q_ref, k_ref, v_ref, dout_ref, marks_ref, turned_ref, cot_ref, gq_ref, gk_ref, wq_ref, wk_ref, wv_ref,
    before_ref, lns_ref, gains_in_ref, grads_ref, dproj_ref, att_ref, gains_ref, ln_ref,
    q_s, k_s, v_s, unit_s, rstd_s, e_s, ds_s, g_s, dq_s, dk_s, dv_s,
):
    group = q_ref.shape[1]
    width = cot_ref.shape[1]
    size = 64
    sid = pos_ref[1]
    step = 256

    def lanes(rows):
        return lax.broadcasted_iota(jnp.int32, (rows, 128), 1)

    same = lax.broadcasted_iota(jnp.int32, (128, 128), 0) // size == lax.broadcasted_iota(jnp.int32, (128, 128), 1) // size
    ones = jnp.where(same, 1.0, 0.0).astype(BF16)

    for r in range(0, group, step):
        rows = slice(r, r + step)
        low = lanes(step) < size
        marks = marks_ref[rows, :].astype(F32)
        away = (marks - 1.0) * EXCLUDE
        v = v_ref[0, rows, :].astype(F32)
        scaled = []
        for n, (raw_ref, gain_ref) in enumerate(((q_ref, gq_ref), (k_ref, gk_ref))):
            raw = raw_ref[0, rows, :]
            center = raw.astype(F32) - dot_nn(raw, ones) * (1.0 / size)
            rstd = lax.rsqrt(split_dot(center * center, ones) * (1.0 / size) + EPS)
            unit = center * rstd
            unit_s[n, rows, :] = unit
            rstd_s[n, rows, :] = rstd
            scaled.append(unit * gain_ref[...])
        for h in range(2):
            mine = low if h == 0 else jnp.logical_not(low)
            q_s[h, rows, :] = jnp.where(mine, scaled[0], marks).astype(BF16)
            k_s[h, rows, :] = jnp.where(mine, scaled[1], away).astype(BF16)
            v_s[h, rows, :] = jnp.where(mine, v, 1.0).astype(BF16)

    block = 256
    for h in range(2):
        for first, count in ((0, RUN), (RUN, group - RUN)):
            span = slice(first, first + count)
            for i in range(0, count, block):
                rows = slice(first + i, first + i + block)
                scores = dot_nt(q_s[h, rows, :], k_s[h, span, :])
                e_s[h, i : i + block, 0:count] = jnp.exp2(scores * SCORE_SCALE).astype(BF16)
            for i in range(0, count, block):
                rows = slice(first + i, first + i + block)
                lane = lanes(block)
                mine = (lane < size) if h == 0 else (lane >= size)
                spare = size if h == 0 else 0
                outs = dot_nn(e_s[h, i : i + block, 0:count], v_s[h, span, :])
                inverse = 1.0 / pltpu.roll(outs, size, 1)
                attended = outs * inverse
                grad_low = (dout_ref[rows, :].astype(F32) * inverse).astype(BF16).astype(F32)
                centre = split_dot(jnp.where(mine, grad_low * attended, 0.0), jnp.ones((128, 128), BF16))
                centre_high = centre.astype(BF16).astype(F32)
                extra = jnp.where(lane == spare, -centre_high, jnp.where(lane == spare + 1, centre_high - centre, 0.0))
                grad_ext = jnp.where(mine, grad_low, extra).astype(BF16)
                g_s[h, rows, :] = grad_ext
                if h == 0:
                    att_ref[rows, :] = attended.astype(BF16)
                else:
                    att_ref[rows, :] = jnp.where(mine, attended, att_ref[rows, :].astype(F32)).astype(BF16)
                d_probs = dot_nt(grad_ext, v_s[h, span, :])
                ds_s[h, i : i + block, 0:count] = (e_s[h, i : i + block, 0:count].astype(F32) * d_probs).astype(BF16)
            dq_s[h, span, :] = dot_nn(ds_s[h, 0:count, 0:count], k_s[h, span, :])
            dk_s[h, span, :] = dot_tn(ds_s[h, 0:count, 0:count], q_s[h, span, :])
            dv_s[h, span, :] = dot_tn(e_s[h, 0:count, 0:count], g_s[h, span, :])

    for r in range(0, group, step):
        rows = slice(r, r + step)
        low = lanes(step) < size
        for n, (grad_s, gain_ref) in enumerate(((dq_s, gq_ref), (dk_s, gk_ref))):
            unit, rstd = unit_s[n, rows, :], rstd_s[n, rows, :]
            grad = jnp.where(low, grad_s[0, rows, :], grad_s[1, rows, :]) * 0.125
            part = jnp.sum((grad * unit).reshape(step // 8, 8, 128), axis=0)
            if r == 0:
                gains_ref[8 * n : 8 * (n + 1), :] = gains_in_ref[8 * n : 8 * (n + 1), :] + part
            else:
                gains_ref[8 * n : 8 * (n + 1), :] += part
            grad = grad * gain_ref[...]
            mean = split_dot(grad, ones) * (1.0 / size)
            slope = split_dot(grad * unit, ones) * (1.0 / size)
            dproj_ref[rows, 128 * n : 128 * (n + 1)] = (rstd * (grad - mean - unit * slope)).astype(BF16)
        dproj_ref[rows, 256:384] = jnp.where(low, dv_s[0, rows, :], dv_s[1, rows, :]).astype(BF16)

    rows = width // BLOCKS
    part = 384
    for j in range(0, width, part):
        grad_in = dot_nn(turned_ref[j : j + part, :], dproj_ref[...])
        terms = lns_ref[:, j : j + part]
        for n, w_ref in enumerate((wq_ref, wk_ref, wv_ref)):
            terms += row_sums(grad_in[:, 128 * n : 128 * (n + 1)] * w_ref[j : j + part, :].astype(F32))
        ln_ref[:, j : j + part] = terms
        for i in range(part // rows):
            grads_ref[(j // rows + i) ^ sid, 0:rows, :] = grad_in[i * rows : (i + 1) * rows].astype(BF16)
    grad_out = dot_tn(att_ref[...], cot_ref[...])
    few = 128 // BLOCKS
    for i in range(BLOCKS):
        piece = grad_out[i * few : (i + 1) * few]
        piece = jnp.concatenate([piece[:, :384], piece[:, 384:]], axis=0)
        grads_ref[i ^ sid, rows : rows + 2 * few, :] = piece.astype(BF16)
    rows += 2 * few
    if grads_ref.shape[1] > rows:
        gains = jnp.sum(gains_ref[...].reshape(2, 8, 128), axis=1)
        gains = gains + pltpu.roll(gains, size, 1)
        gains = jnp.where(lanes(1) < size, gains[0:1], gains[1:2])
        small = [ln_ref[0:1, 0:384], ln_ref[0:1, 384:768], jnp.concatenate([gains, jnp.zeros((1, 256), F32)], axis=1)]
        small = jnp.concatenate(small + [jnp.zeros((5, 384), F32)], axis=0)
        for i in range(BLOCKS):
            grads_ref[i ^ sid, rows : rows + 8, :] = (small if i == 0 else jnp.zeros_like(small)).astype(BF16)


def attend(pos, pair, projected, gain_q, gain_k, w_in, before, lns, gains):
    normed, turned, cot, marks, raw, dout, _ = projected
    group, width = normed.shape
    last = pair == 2
    rows = width // BLOCKS + 16 + 8 * last
    cols = 384 if last else 768
    alias = {13: 0} if pair == 1 else {}
    before_spec = pl.BlockSpec(memory_space=pl.ANY)

    def whole(shape):
        return pl.BlockSpec(shape, lambda i, pos: (0,) * len(shape))

    raw_specs = [pl.BlockSpec((1, group, 128), lambda i, pos, n=n: (n, 0, pair)) for n in range(3)]
    return pl.pallas_call(
        attend_body,
        out_shape=(
            jax.ShapeDtypeStruct((BLOCKS, rows, cols), BF16),
            jax.ShapeDtypeStruct((group, 384), BF16),
            jax.ShapeDtypeStruct((group, 128), BF16),
            jax.ShapeDtypeStruct((16, 128), F32),
            jax.ShapeDtypeStruct((8, width), F32),
        ),
        grid_spec=pltpu.PrefetchScalarGridSpec(
            num_scalar_prefetch=1,
            grid=(1,),
            in_specs=raw_specs
            + [
                pl.BlockSpec((group, 128), lambda i, pos: (0, pair)),
                whole(marks.shape),
                whole(turned.shape),
                whole(cot.shape),
                whole((1, 128)),
                whole((1, 128)),
            ]
            + [pl.BlockSpec((width, 128), lambda i, pos, n=n: (0, 6 * n + 3 * pos[0] + pair)) for n in range(3)]
            + [before_spec, whole((8, width)), whole((16, 128))],
            out_specs=[
                pl.BlockSpec((BLOCKS, rows, 384), lambda i, pos: (0, 0, 1 if pair == 1 else 0)),
                whole((group, 384)),
                whole((group, 128)),
                whole((16, 128)),
                whole((8, width)),
            ],
            scratch_shapes=[
                pltpu.VMEM((2, group, 128), BF16),
                pltpu.VMEM((2, group, 128), BF16),
                pltpu.VMEM((2, group, 128), BF16),
                pltpu.VMEM((2, group, 128), F32),
                pltpu.VMEM((2, group, 128), F32),
                pltpu.VMEM((2, RUN, RUN), BF16),
                pltpu.VMEM((2, RUN, RUN), BF16),
                pltpu.VMEM((2, group, 128), BF16),
                pltpu.VMEM((2, group, 128), F32),
                pltpu.VMEM((2, group, 128), F32),
                pltpu.VMEM((2, group, 128), F32),
            ],
        ),
        input_output_aliases=alias,
        compiler_params=pltpu.CompilerParams(vmem_limit_bytes=VMEM),
        cost_estimate=SHORT,
        name=f"attend{pair}",
    )(pos, raw, raw, raw, dout, marks, turned, cot, gain_q, gain_k, w_in, w_in, w_in, before, lns, gains)


def combine_body(pos_ref, start_ref, *refs):
    weights, dprojs, atts = refs[0:12], refs[12:15], refs[15:18]
    part_ref, both_s = refs[18:]
    group, width = atts[0].shape[0], weights[3].shape[1]
    bo = sum(dot_nn(atts[p][...], weights[4 * p + 3][...]) for p in range(3))
    both_s[0:group, 0:width] = bo.astype(BF16)
    dn = None
    for p in range(3):
        for n in range(3):
            term = dot_nt(dprojs[p][:, 128 * n : 128 * (n + 1)], weights[4 * p + n][...])
            dn = term if dn is None else dn + term
    both_s[0:group, width : 2 * width] = dn.astype(BF16)
    block = 128
    both_s[group : group + block, :] = both_s[0:block, :]
    back = group - start_ref[0]
    high, rest = back // block, back % block
    row = lax.broadcasted_iota(jnp.int32, (block, 2 * block), 0)
    col = lax.broadcasted_iota(jnp.int32, (block, 2 * block), 1)
    shift = jnp.where(col == row + rest, 1.0, 0.0).astype(BF16)
    half = group // (2 * block)
    for i in range(group // block):
        at = pl.multiple_of(((i + high) % (group // block)) * block, block)
        moved = dot_nn(shift, both_s[pl.ds(at, 2 * block), :]).astype(BF16)
        part_ref[i // half, (i % half) * block : (i % half + 1) * block, :] = moved


def combine(pos, start, w_in, w_attn_out, dprojs, atts):
    group, width = atts[0].shape[0], w_attn_out.shape[1]

    def whole(shape):
        return pl.BlockSpec(shape, lambda i, pos, start: (0,) * len(shape))

    weights, specs = [], []
    for p in range(3):
        for n in range(3):
            weights.append(w_in)
            specs.append(pl.BlockSpec((width, 128), lambda i, pos, start, p=p, n=n: (0, 6 * n + 3 * pos[0] + p)))
        weights.append(w_attn_out)
        specs.append(pl.BlockSpec((128, width), lambda i, pos, start, p=p: (3 * pos[0] + p, 0)))
    out = (2, group // 2, 2 * width)
    return pl.pallas_call(
        combine_body,
        out_shape=jax.ShapeDtypeStruct(out, BF16),
        grid_spec=pltpu.PrefetchScalarGridSpec(
            num_scalar_prefetch=2,
            grid=(1,),
            in_specs=specs + [whole((group, 384))] * 3 + [whole((group, 128))] * 3,
            out_specs=whole(out),
            scratch_shapes=[pltpu.VMEM((group + 128, 2 * width), BF16)],
        ),
        cost_estimate=SHORT,
        compiler_params=pltpu.CompilerParams(vmem_limit_bytes=VMEM),
        name="combine",
    )(pos, start, *weights, *dprojs, *atts)


def finish_body(
    pos_ref, image_ref, cot_ref, gain_ref, here_ref, there_ref, joined_ref, got_ref, out_ref, grad_ref
):
    tokens, width = image_ref.shape
    step = 64
    stays = pos_ref[0] == pos_ref[2]

    def put(source):
        for r in range(0, tokens, step):
            rows = slice(r, r + step)
            x = image_ref[rows, :].astype(F32)
            total = here_ref[rows, :] + (there_ref[rows, :].astype(F32) + source[rows, :].astype(F32))
            out_ref[rows, :] = (x + total[:, 0:width]).astype(BF16)
            center = x - jnp.mean(x, axis=-1, keepdims=True)
            rstd = lax.rsqrt(jnp.mean(center * center, axis=-1, keepdims=True) + EPS)
            scaled = center * rstd
            grad = total[:, width : 2 * width] * gain_ref[...]
            mean = jnp.mean(grad, axis=-1, keepdims=True)
            slope = jnp.mean(grad * scaled, axis=-1, keepdims=True)
            grad_ref[rows, :] = cot_ref[rows, :].astype(F32) + rstd * (grad - mean - scaled * slope)

    pl.when(stays)(lambda: put(joined_ref))
    pl.when(jnp.logical_not(stays))(lambda: put(got_ref))


def finish(pos, image_in, cotangent, ln_gain, here, there, joined, got):
    tokens, width = image_in.shape
    vmem = pl.BlockSpec(memory_space=pltpu.VMEM)
    return pl.pallas_call(
        finish_body,
        out_shape=(jax.ShapeDtypeStruct((tokens, width), BF16), jax.ShapeDtypeStruct((tokens, width), F32)),
        in_specs=[pl.BlockSpec(memory_space=pltpu.SMEM)] + [vmem] * 7,
        out_specs=(vmem, vmem),
        compiler_params=pltpu.CompilerParams(vmem_limit_bytes=VMEM),
        cost_estimate=SHORT,
        name="finish",
    )(pos, image_in, cotangent, ln_gain, here, there, joined, got)


def exchange(value, mask):
    count = lax.axis_size(AXES)
    return lax.ppermute(value, AXES, [(i, i ^ mask) for i in range(count)])


def add_low(left, right):
    return (left.astype(F32) + right.astype(F32)).astype(BF16)


class Order:
    def __init__(self, places):
        self.places = places

    def after(self, value):
        value, self.places = lax.optimization_barrier((value, self.places))
        return value


def travel(order, halves, masks, rest):
    for mask in masks:
        got = exchange(halves[1], mask)
        yield
        chunk = order.after(add_low(halves[0], order.after(got)))
        middle = chunk.shape[0] // 2
        halves = chunk[:middle], chunk[middle:]
    for mask in rest:
        chunk = order.after(add_low(chunk, exchange(chunk, mask)))
    for mask in reversed(masks):
        got = exchange(chunk, mask)
        yield
        chunk = order.after(jnp.concatenate([chunk, order.after(got)], axis=0))
    mate = exchange(chunk, 2)
    yield
    yield chunk, order.after(mate)


def spread_mlp_body(pos_ref, own_ref, mate_ref, *refs):
    out_ref, in_ref = refs[-2:]
    sid = pos_ref[1]
    rows = own_ref.shape[1] // 2
    side, quarter = pl.program_id(0), pl.program_id(1)

    def put(source):
        for i in range(4):
            at = (4 * quarter + i) ^ sid
            out_ref[i * rows : (i + 1) * rows, :] = source[at, 0:rows, :].astype(F32)
            in_ref[i * rows : (i + 1) * rows, :] = source[at, rows : 2 * rows, :].astype(F32)

    pl.when(side == 0)(lambda: put(own_ref))
    pl.when(side == 1)(lambda: put(mate_ref))


def spread_mlp(pos, own, mate, part, shapes, before):
    blocks, rows2, width = own.shape
    whole = pl.BlockSpec(own.shape, lambda r, g, pos: (0, 0, 0))
    return pl.pallas_call(
        spread_mlp_body,
        out_shape=tuple(jax.ShapeDtypeStruct(s, F32) for s in shapes),
        grid_spec=pltpu.PrefetchScalarGridSpec(
            num_scalar_prefetch=1,
            grid=(2, 4),
            in_specs=[whole, whole] + [pl.BlockSpec(memory_space=pl.ANY)] * len(before),
            out_specs=[
                pl.BlockSpec((width // 4, width), lambda r, g, pos: (4 * (2 * (r ^ pos[0]) + part) + g, 0)),
                pl.BlockSpec((width // 4, width), lambda r, g, pos: (g, 3 + 2 * (r ^ pos[0]) + part)),
            ],
        ),
        input_output_aliases={3 + i: out for i, out in enumerate(before)},
        compiler_params=pltpu.CompilerParams(dimension_semantics=("arbitrary", "arbitrary"), vmem_limit_bytes=VMEM),
        cost_estimate=SHORT,
        name=f"spread_mlp{part}",
    )(pos, own, mate, *before.values())


def spread_attention_body(pos_ref, own_ref, mate_ref, *refs):
    in_ref, out_ref = refs[-3:-1] if own_ref.shape[1] > 64 else refs[-2:]
    sid = pos_ref[1]
    blocks = own_ref.shape[0]
    rows = 48
    side, kind = pl.program_id(0), pl.program_id(2)

    def put(source):
        from_col = pl.ds(pl.multiple_of(128 * kind, 128), 128)
        for i in range(blocks):
            in_ref[i * rows : (i + 1) * rows, :] = source[i ^ sid, 0:rows, from_col].astype(F32)

        @pl.when(kind == 0)
        def _():
            for i in range(blocks):
                piece = source[i ^ sid, rows : rows + 16, :].astype(F32)
                out_ref[8 * i : 8 * (i + 1), 0:384] = piece[0:8]
                out_ref[8 * i : 8 * (i + 1), 384:768] = piece[8:16]

    pl.when(side == 0)(lambda: put(own_ref))
    pl.when(side == 1)(lambda: put(mate_ref))
    if own_ref.shape[1] > 64:
        refs[-1][...] = own_ref[sid, 64:72, :].astype(F32) + mate_ref[sid, 64:72, :].astype(F32)


def spread_attention(pos, own, mate, pairs, shapes, before):
    rows = own.shape[1]
    width = shapes[1][0]
    base = pairs[0]
    block = pl.BlockSpec((BLOCKS, rows, 384), lambda r, p, k, pos: (0, 0, p))
    out_shape = [jax.ShapeDtypeStruct(s, F32) for s in shapes]
    out_specs = [
        pl.BlockSpec((width, 128), lambda r, p, k, pos: (0, 6 * k + 3 * (r ^ pos[0]) + base + p)),
        pl.BlockSpec((128, width), lambda r, p, k, pos: (3 * (r ^ pos[0]) + base + p, 0)),
    ]
    if rows > 64:
        out_shape.append(jax.ShapeDtypeStruct((8, 384), F32))
        out_specs.append(pl.BlockSpec((8, 384), lambda r, p, k, pos: (0, 0)))
    return pl.pallas_call(
        spread_attention_body,
        out_shape=tuple(out_shape),
        grid_spec=pltpu.PrefetchScalarGridSpec(
            num_scalar_prefetch=1,
            grid=(2, len(pairs), 3),
            in_specs=[block, block] + [pl.BlockSpec(memory_space=pl.ANY)] * len(before),
            out_specs=out_specs,
        ),
        input_output_aliases={3 + i: out for i, out in enumerate(before)},
        compiler_params=pltpu.CompilerParams(
            dimension_semantics=("arbitrary",) * 3, vmem_limit_bytes=VMEM
        ),
        cost_estimate=SHORT,
        name=f"spread_attention{base}",
    )(pos, own, mate, *before.values())


def per_device(image_in, ln_gain, w_in, q_gain, k_gain, w_attn_out, w_mlp_out, cotangent, image_ids):
    tokens, width = image_in.shape
    count = lax.axis_size(AXES)
    index = lax.axis_index(AXES)
    side = index & 1
    core = (index >> 1) & 1
    others = [1 << k for k in range(2, count.bit_length() - 1)]
    y, z, far = others[:3]
    masks = {
        "m0": [z, y, 1, far],
        "m1": [1, y, z, far],
        "a0": [z, y, 1, far],
        "a1": [y, z, 1, far],
    }
    rest = others[3:]
    crossing = [(i, i ^ 3) for i in range(count) if i & 3 in (1, 2)]

    def place(masks):
        sid = jnp.int32(0)
        for mask in masks:
            sid = 2 * sid + ((index & mask) != 0).astype(jnp.int32)
        return jnp.stack([core, sid, side])

    order = Order({name: place(masks[name]) for name in masks})
    trips, ended = {}, {}

    def chunk(name, keep, send):
        trips[name] = travel(order, (keep, order.after(send)), masks[name], rest)
        next(trips[name])

    def hop(*names):
        for name in names:
            ended[name] = next(trips[name])

    def call(kernel, name, *values):
        return order.after(kernel(order.places[name], *values))

    gain_row = ln_gain.reshape(1, width)
    gain_q = jnp.concatenate([q_gain, q_gain]).reshape(1, 128)
    gain_k = jnp.concatenate([k_gain, k_gain]).reshape(1, 128)
    ids = lax.dynamic_slice(image_ids, (0, side * tokens), (1, tokens))
    packed = order.after(prep(ids, image_in, cotangent, gain_row))
    beside = exchange(packed, 2)
    crossed = lax.ppermute(packed, AXES, crossing)
    beside = order.after(beside)
    *grads, here, there, ln0 = call(mlp, "m0", packed, beside, w_in, w_mlp_out, 0, ())
    chunk("m0", *grads)
    *grads, here, there, ln1 = call(mlp, "m1", packed, beside, w_in, w_mlp_out, 1, (here, there))
    chunk("m1", *grads)
    swapped = order.after(jnp.where(core == side, packed, order.after(crossed)))
    mate = exchange(swapped, 2)
    hop("m0")
    mate = order.after(mate)
    projected = call(project, "a0", swapped, mate, w_in, w_attn_out)
    empty = jnp.zeros((8, 128), BF16)
    sums = (ln0 + ln1, jnp.zeros((16, 128), F32))
    first = call(attend, "a0", 0, projected, gain_q, gain_k, w_in, empty, *sums)
    hop("m1", "m0")
    there = exchange(there, 2)
    second = call(attend, "a0", 1, projected, gain_q, gain_k, w_in, first[0], first[4], first[3])
    hop("m1", "m0")
    chunk("a0", second[0][:8], second[0][8:])
    there = order.after(there)
    third = call(attend, "a1", 2, projected, gain_q, gain_k, w_in, empty, second[4], second[3])
    hop("m1", "m0")
    chunk("a1", third[0][:8], third[0][8:])
    pieces = (first, second, third)
    parts = call(
        combine, "a0", projected[6], w_in, w_attn_out, [p[1] for p in pieces], [p[2] for p in pieces]
    )
    hop("a0", "a1", "m1")
    got = exchange(parts[1], 2)
    hop("m0", "a1", "a0")
    joined = order.after(add_low(parts[0], order.after(got)))
    got = lax.ppermute(joined, AXES, crossing)
    hop("m1", "m0", "a1", "a0", "m1", "a1", "a0", "m0", "a1", "a0")
    got = order.after(got)
    block_out, grad_image = call(
        finish, "a0", image_in, cotangent, gain_row, here, there, joined, got
    )
    hop("m1", "a1", "a0", "a0", "m0", "a1", "m1", "m0")
    of_mlp, of_attention = (w_mlp_out.shape, w_in.shape), (w_in.shape, w_attn_out.shape)
    grad_mlp_w, grad_win = call(spread_mlp, "m0", *ended["m0"], 0, of_mlp, {})
    hop("a1", "a0", "m1")
    grad_mlp_w, grad_win = call(spread_mlp, "m1", *ended["m1"], 1, of_mlp, {0: grad_mlp_w, 1: grad_win})
    hop("a1")
    before = {0: grad_win}
    grad_win, grad_attn_w, small = call(spread_attention, "a1", *ended["a1"], (2,), of_attention, before)
    hop("a0")
    before = {0: grad_win, 1: grad_attn_w}
    grad_win, grad_attn_w = call(spread_attention, "a0", *ended["a0"], (0, 1), of_attention, before)
    small = small.reshape(-1)
    return (
        block_out, grad_image, small[0:width] / ln_gain, grad_win, small[width : width + 64],
        small[width + 64 : width + 128], grad_attn_w, grad_mlp_w,
    )


def solution(mesh):
    tokens = P(("seq", "head"), None)
    return jax.shard_map(
        per_device,
        mesh=mesh,
        in_specs=(tokens, P(), P(), P(), P(), P(), P(), tokens, P("seq", None)),
        out_specs=(tokens, tokens, P(), P(), P(), P(), P(), P()),
        check_vma=False,
    )
```

```python
import functools
import math

import jax
import jax.numpy as jnp
from jax import lax
from jax.experimental import pallas as pl
from jax.experimental.pallas import tpu as pltpu
from jax.sharding import PartitionSpec as P

F32 = jnp.float32
BF16 = jnp.bfloat16
EPS = 1e-06
AXES = ("seq", "head")
VMEM = 32 << 20
BLOCKS = 16
EXCLUDE = 32768.0
SHORT = pl.CostEstimate(flops=1, bytes_accessed=1, transcendentals=0)
SCORE_SCALE = 0.125 * math.log2(math.e)


def dot_nn(a, b):
    return lax.dot_general(a, b, (((1,), (0,)), ((), ())), preferred_element_type=F32)


def dot_nt(a, b):
    return lax.dot_general(a, b, (((1,), (1,)), ((), ())), preferred_element_type=F32)


def dot_tn(a, b):
    return lax.dot_general(a, b, (((0,), (0,)), ((), ())), preferred_element_type=F32)


def row_sums(x):
    ones = jnp.ones((8, x.shape[1]), BF16)
    high = x.astype(BF16)
    low = (x - high.astype(F32)).astype(BF16)
    return dot_nt(ones, high) + dot_nt(ones, low)


def prep_body(ids_ref, image_ref, cot_ref, gain_ref, out_ref):
    tokens, width = image_ref.shape
    step = 64
    for r in range(0, tokens, step):
        x = image_ref[r : r + step, :].astype(F32)
        center = x - jnp.mean(x, axis=-1, keepdims=True)
        spread = jnp.mean(center * center, axis=-1, keepdims=True)
        out_ref[r : r + step, 0:width] = (center * lax.rsqrt(spread + EPS) * gain_ref[...]).astype(BF16)
    out_ref[:, width : 2 * width] = cot_ref[...]
    ids = ids_ref[...]
    image = lax.broadcasted_iota(jnp.int32, (128, tokens), 0) & 63
    marks = jnp.where(image == ids, 1.0, 0.0).astype(F32)
    out_ref[:, 2 * width :] = jnp.transpose(marks).astype(BF16)


def prep(ids, image_in, cotangent, ln_gain):
    tokens, width = image_in.shape
    return pl.pallas_call(
        prep_body,
        out_shape=jax.ShapeDtypeStruct((tokens, 2 * width + 128), BF16),
        cost_estimate=SHORT,
        name="prep",
    )(ids, image_in, cotangent, ln_gain)


def mlp_body(
    pos_ref, own_ref, mate_ref, win_ref, wout_ref, *refs,
):
    before = refs[:-11]
    keep_ref, send_ref, here_ref, there_ref, ln_ref, normed_s, cot_s, up_s, dact_s, act_s, dup_s = refs[-11:]
    tokens = own_ref.shape[0]
    width = wout_ref.shape[1]
    sid = pos_ref[1]
    for i, ref in enumerate((own_ref, mate_ref)):
        normed_s[i * tokens : (i + 1) * tokens, :] = ref[:, 0:width]
        cot_s[i * tokens : (i + 1) * tokens, :] = ref[:, width : 2 * width]
    up_s[...] = dot_nn(normed_s[...], win_ref[...])
    dact_s[...] = dot_nt(cot_s[...], wout_ref[...])
    step = 32

    def gelu_rows(i, carry):
        rows = pl.ds(pl.multiple_of(i * step, step), step)
        up = up_s[rows, :]
        cdf = 0.5 * (1.0 + lax.erf(up * math.sqrt(0.5)))
        pdf = jnp.exp(-0.5 * up * up) * (1.0 / math.sqrt(2.0 * math.pi))
        act_s[rows, :] = (up * cdf).astype(BF16)
        dup_s[rows, :] = (dact_s[rows, :] * (cdf + up * pdf)).astype(BF16)
        return carry

    lax.fori_loop(0, 2 * tokens // step, gelu_rows, 0)
    rows = width // BLOCKS
    part = width // 2
    for other, ref in enumerate((keep_ref, send_ref)):
        cols = pl.ds(pl.multiple_of((sid // (BLOCKS // 2) ^ other) * part, part), part)
        grad_out = dot_tn(act_s[:, cols], cot_s[...])
        grad_in = dot_tn(normed_s[:, cols], dup_s[...])
        ln_ref[:, cols] = row_sums(grad_in * win_ref[cols, :].astype(F32))
        for i in range(BLOCKS // 2):
            where = i ^ (sid % (BLOCKS // 2))
            ref[where, 0:rows, :] = grad_out[i * rows : (i + 1) * rows].astype(BF16)
            ref[where, rows : 2 * rows, :] = grad_in[i * rows : (i + 1) * rows].astype(BF16)
    for side in range(2):
        cols = slice(side * width, (side + 1) * width)
        here = dot_nt(dup_s[0:tokens, :], win_ref[...]) if side else dot_nn(act_s[0:tokens, :], wout_ref[...])
        there = dot_nt(dup_s[tokens:, :], win_ref[...]) if side else dot_nn(act_s[tokens:, :], wout_ref[...])
        if before:
            here += before[0][:, cols]
            there += before[1][:, cols].astype(F32)
        here_ref[:, cols] = here
        there_ref[:, cols] = there.astype(BF16)


def mlp(pos, own, mate, w_in, w_mlp_out, part, before):
    tokens = own.shape[0]
    width = w_mlp_out.shape[1]
    rows = width // BLOCKS

    def whole(shape):
        return pl.BlockSpec(shape, lambda i, pos: (0,) * len(shape))

    half = (BLOCKS // 2, 2 * rows, width)
    outs = [half, half, (tokens, 2 * width), (tokens, 2 * width), (8, width)]
    return pl.pallas_call(
        mlp_body,
        out_shape=tuple(jax.ShapeDtypeStruct(s, t) for s, t in zip(outs, (BF16, BF16, F32, BF16, F32))),
        grid_spec=pltpu.PrefetchScalarGridSpec(
            num_scalar_prefetch=1,
            grid=(1,),
            in_specs=[
                whole(own.shape),
                whole(own.shape),
                pl.BlockSpec((width, width), lambda i, pos: (0, 3 + 2 * pos[0] + part)),
                pl.BlockSpec((width, width), lambda i, pos: (2 * pos[0] + part, 0)),
            ]
            + [whole(x.shape) for x in before],
            out_specs=[whole(s) for s in outs],
            scratch_shapes=[pltpu.VMEM((2 * tokens, width), t) for t in (BF16, BF16, F32, F32, BF16, BF16)],
        ),
        compiler_params=pltpu.CompilerParams(dimension_semantics=("arbitrary",), vmem_limit_bytes=54 << 20),
        cost_estimate=SHORT,
        name=f"mlp{part}",
    )(pos, own, mate, w_in, w_mlp_out, *before)


RUN = 768


def project_body(
    pos_ref, own_ref, mate_ref, wq_ref, wk_ref, wv_ref, wo_ref,
    normed_ref, turned_ref, cot_ref, marks_ref, raw_ref, dout_ref, start_ref, twice_s,
):
    tokens, packed = own_ref.shape
    width = wo_ref.shape[1]
    group = 2 * tokens
    block = 128
    twice_s[0:tokens, :] = own_ref[...]
    twice_s[tokens:group, :] = mate_ref[...]
    twice_s[group : group + block, :] = own_ref[0:block, :]
    marks = twice_s[0:group, 2 * width :]
    held = dot_nn(jnp.ones((8, group), BF16), marks)
    lane = lax.broadcasted_iota(jnp.int32, (8, 128), 1)
    chosen = jnp.where(jnp.logical_and(held == float(RUN), lane < 64), 1.0, 0.0).astype(BF16)
    inside = dot_nt(chosen, marks)
    before = pltpu.roll(inside, 1, 1)
    place = lax.broadcasted_iota(jnp.int32, (8, group), 1).astype(F32)
    opens = jnp.where(jnp.logical_and(inside > 0.5, before < 0.5), place, 0.0)
    start = jnp.sum(opens[0:1, :]).astype(jnp.int32)
    start_ref[0] = start
    high, rest = start // block, start % block
    row = lax.broadcasted_iota(jnp.int32, (block, 2 * block), 0)
    col = lax.broadcasted_iota(jnp.int32, (block, 2 * block), 1)
    shift = jnp.where(col == row + rest, 1.0, 0.0).astype(BF16)
    for i in range(group // block):
        at = pl.multiple_of(((i + high) % (group // block)) * block, block)
        moved = dot_nn(shift, twice_s[pl.ds(at, 2 * block), :]).astype(BF16)
        rows = slice(i * block, (i + 1) * block)
        normed_ref[rows, :] = moved[:, 0:width]
        cot_ref[rows, :] = moved[:, width : 2 * width]
        marks_ref[rows, :] = moved[:, 2 * width :]
    for n, w_ref in enumerate((wq_ref, wk_ref, wv_ref)):
        raw_ref[n, :, :] = dot_nn(normed_ref[...], w_ref[...]).astype(BF16)
    dout_ref[...] = dot_nt(cot_ref[...], wo_ref[...]).astype(BF16)
    for j in range(0, width, 128):
        turned_ref[j : j + 128, :] = jnp.transpose(normed_ref[:, j : j + 128].astype(F32)).astype(BF16)


def project(pos, own, mate, w_in, w_attn_out):
    tokens, packed = own.shape
    width = w_attn_out.shape[1]
    group = 2 * tokens
    part = width // 2

    def whole(shape):
        return pl.BlockSpec(shape, lambda i, pos: (0,) * len(shape))

    outs = [(group, width), (width, group), (group, width), (group, 128), (3, group, part), (group, part)]
    return pl.pallas_call(
        project_body,
        out_shape=tuple(jax.ShapeDtypeStruct(s, BF16) for s in outs) + (jax.ShapeDtypeStruct((1,), jnp.int32),),
        grid_spec=pltpu.PrefetchScalarGridSpec(
            num_scalar_prefetch=1,
            grid=(1,),
            in_specs=[
                whole(own.shape),
                whole(own.shape),
                pl.BlockSpec((width, part), lambda i, pos: (0, pos[0])),
                pl.BlockSpec((width, part), lambda i, pos: (0, 2 + pos[0])),
                pl.BlockSpec((width, part), lambda i, pos: (0, 4 + pos[0])),
                pl.BlockSpec((part, width), lambda i, pos: (pos[0], 0)),
            ],
            out_specs=[whole(s) for s in outs] + [pl.BlockSpec(memory_space=pltpu.SMEM)],
            scratch_shapes=[pltpu.VMEM((group + 128, packed), BF16)],
        ),
        cost_estimate=SHORT,
        compiler_params=pltpu.CompilerParams(vmem_limit_bytes=VMEM),
        name="project",
    )(pos, own, mate, w_in, w_in, w_in, w_attn_out)


def split_dot(x, ones):
    high = x.astype(BF16)
    low = (x - high.astype(F32)).astype(BF16)
    return dot_nn(high, ones) + dot_nn(low, ones)


def attend_body(
    pos_ref, q_ref, k_ref, v_ref, dout_ref, marks_ref, turned_ref, cot_ref, gq_ref, gk_ref, wq_ref, wk_ref, wv_ref,
    before_ref, lns_ref, gains_in_ref, grads_ref, dproj_ref, att_ref, gains_ref, ln_ref,
    q_s, k_s, v_s, unit_s, rstd_s, e_s, ds_s, g_s, dq_s, dk_s, dv_s,
):
    group = q_ref.shape[1]
    width = cot_ref.shape[1]
    size = 64
    sid = pos_ref[1]
    step = 256

    def lanes(rows):
        return lax.broadcasted_iota(jnp.int32, (rows, 128), 1)

    same = lax.broadcasted_iota(jnp.int32, (128, 128), 0) // size == lax.broadcasted_iota(jnp.int32, (128, 128), 1) // size
    ones = jnp.where(same, 1.0, 0.0).astype(BF16)

    for r in range(0, group, step):
        rows = slice(r, r + step)
        low = lanes(step) < size
        marks = marks_ref[rows, :].astype(F32)
        away = (marks - 1.0) * EXCLUDE
        v = v_ref[0, rows, :].astype(F32)
        scaled = []
        for n, (raw_ref, gain_ref) in enumerate(((q_ref, gq_ref), (k_ref, gk_ref))):
            raw = raw_ref[0, rows, :]
            center = raw.astype(F32) - dot_nn(raw, ones) * (1.0 / size)
            rstd = lax.rsqrt(split_dot(center * center, ones) * (1.0 / size) + EPS)
            unit = center * rstd
            unit_s[n, rows, :] = unit
            rstd_s[n, rows, :] = rstd
            scaled.append(unit * gain_ref[...])
        for h in range(2):
            mine = low if h == 0 else jnp.logical_not(low)
            q_s[h, rows, :] = jnp.where(mine, scaled[0], marks).astype(BF16)
            k_s[h, rows, :] = jnp.where(mine, scaled[1], away).astype(BF16)
            v_s[h, rows, :] = jnp.where(mine, v, 1.0).astype(BF16)

    block = 256
    for h in range(2):
        for first, count in ((0, RUN), (RUN, group - RUN)):
            span = slice(first, first + count)
            for i in range(0, count, block):
                rows = slice(first + i, first + i + block)
                scores = dot_nt(q_s[h, rows, :], k_s[h, span, :])
                e_s[h, i : i + block, 0:count] = jnp.exp2(scores * SCORE_SCALE).astype(BF16)
            for i in range(0, count, block):
                rows = slice(first + i, first + i + block)
                lane = lanes(block)
                mine = (lane < size) if h == 0 else (lane >= size)
                spare = size if h == 0 else 0
                outs = dot_nn(e_s[h, i : i + block, 0:count], v_s[h, span, :])
                inverse = 1.0 / pltpu.roll(outs, size, 1)
                attended = outs * inverse
                grad_low = (dout_ref[rows, :].astype(F32) * inverse).astype(BF16).astype(F32)
                centre = split_dot(jnp.where(mine, grad_low * attended, 0.0), jnp.ones((128, 128), BF16))
                centre_high = centre.astype(BF16).astype(F32)
                extra = jnp.where(lane == spare, -centre_high, jnp.where(lane == spare + 1, centre_high - centre, 0.0))
                grad_ext = jnp.where(mine, grad_low, extra).astype(BF16)
                g_s[h, rows, :] = grad_ext
                if h == 0:
                    att_ref[rows, :] = attended.astype(BF16)
                else:
                    att_ref[rows, :] = jnp.where(mine, attended, att_ref[rows, :].astype(F32)).astype(BF16)
                d_probs = dot_nt(grad_ext, v_s[h, span, :])
                ds_s[h, i : i + block, 0:count] = (e_s[h, i : i + block, 0:count].astype(F32) * d_probs).astype(BF16)
            dq_s[h, span, :] = dot_nn(ds_s[h, 0:count, 0:count], k_s[h, span, :])
            dk_s[h, span, :] = dot_tn(ds_s[h, 0:count, 0:count], q_s[h, span, :])
            dv_s[h, span, :] = dot_tn(e_s[h, 0:count, 0:count], g_s[h, span, :])

    for r in range(0, group, step):
        rows = slice(r, r + step)
        low = lanes(step) < size
        for n, (grad_s, gain_ref) in enumerate(((dq_s, gq_ref), (dk_s, gk_ref))):
            unit, rstd = unit_s[n, rows, :], rstd_s[n, rows, :]
            grad = jnp.where(low, grad_s[0, rows, :], grad_s[1, rows, :]) * 0.125
            part = jnp.sum((grad * unit).reshape(step // 8, 8, 128), axis=0)
            if r == 0:
                gains_ref[8 * n : 8 * (n + 1), :] = gains_in_ref[8 * n : 8 * (n + 1), :] + part
            else:
                gains_ref[8 * n : 8 * (n + 1), :] += part
            grad = grad * gain_ref[...]
            mean = split_dot(grad, ones) * (1.0 / size)
            slope = split_dot(grad * unit, ones) * (1.0 / size)
            dproj_ref[rows, 128 * n : 128 * (n + 1)] = (rstd * (grad - mean - unit * slope)).astype(BF16)
        dproj_ref[rows, 256:384] = jnp.where(low, dv_s[0, rows, :], dv_s[1, rows, :]).astype(BF16)

    rows = width // BLOCKS
    part = 384
    for j in range(0, width, part):
        grad_in = dot_nn(turned_ref[j : j + part, :], dproj_ref[...])
        terms = lns_ref[:, j : j + part]
        for n, w_ref in enumerate((wq_ref, wk_ref, wv_ref)):
            terms += row_sums(grad_in[:, 128 * n : 128 * (n + 1)] * w_ref[j : j + part, :].astype(F32))
        ln_ref[:, j : j + part] = terms
        for i in range(part // rows):
            grads_ref[(j // rows + i) ^ sid, 0:rows, :] = grad_in[i * rows : (i + 1) * rows].astype(BF16)
    grad_out = dot_tn(att_ref[...], cot_ref[...])
    few = 128 // BLOCKS
    for i in range(BLOCKS):
        piece = grad_out[i * few : (i + 1) * few]
        piece = jnp.concatenate([piece[:, :384], piece[:, 384:]], axis=0)
        grads_ref[i ^ sid, rows : rows + 2 * few, :] = piece.astype(BF16)
    rows += 2 * few
    if grads_ref.shape[1] > rows:
        gains = jnp.sum(gains_ref[...].reshape(2, 8, 128), axis=1)
        gains = gains + pltpu.roll(gains, size, 1)
        gains = jnp.where(lanes(1) < size, gains[0:1], gains[1:2])
        small = [ln_ref[0:1, 0:384], ln_ref[0:1, 384:768], jnp.concatenate([gains, jnp.zeros((1, 256), F32)], axis=1)]
        small = jnp.concatenate(small + [jnp.zeros((5, 384), F32)], axis=0)
        for i in range(BLOCKS):
            grads_ref[i ^ sid, rows : rows + 8, :] = (small if i == 0 else jnp.zeros_like(small)).astype(BF16)


def attend(pos, pair, projected, gain_q, gain_k, w_in, before, lns, gains):
    normed, turned, cot, marks, raw, dout, _ = projected
    group, width = normed.shape
    last = pair == 2
    rows = width // BLOCKS + 16 + 8 * last
    cols = 384 if last else 768
    alias = {13: 0} if pair == 1 else {}
    before_spec = pl.BlockSpec(memory_space=pl.ANY)

    def whole(shape):
        return pl.BlockSpec(shape, lambda i, pos: (0,) * len(shape))

    raw_specs = [pl.BlockSpec((1, group, 128), lambda i, pos, n=n: (n, 0, pair)) for n in range(3)]
    return pl.pallas_call(
        attend_body,
        out_shape=(
            jax.ShapeDtypeStruct((BLOCKS, rows, cols), BF16),
            jax.ShapeDtypeStruct((group, 384), BF16),
            jax.ShapeDtypeStruct((group, 128), BF16),
            jax.ShapeDtypeStruct((16, 128), F32),
            jax.ShapeDtypeStruct((8, width), F32),
        ),
        grid_spec=pltpu.PrefetchScalarGridSpec(
            num_scalar_prefetch=1,
            grid=(1,),
            in_specs=raw_specs
            + [
                pl.BlockSpec((group, 128), lambda i, pos: (0, pair)),
                whole(marks.shape),
                whole(turned.shape),
                whole(cot.shape),
                whole((1, 128)),
                whole((1, 128)),
            ]
            + [pl.BlockSpec((width, 128), lambda i, pos, n=n: (0, 6 * n + 3 * pos[0] + pair)) for n in range(3)]
            + [before_spec, whole((8, width)), whole((16, 128))],
            out_specs=[
                pl.BlockSpec((BLOCKS, rows, 384), lambda i, pos: (0, 0, 1 if pair == 1 else 0)),
                whole((group, 384)),
                whole((group, 128)),
                whole((16, 128)),
                whole((8, width)),
            ],
            scratch_shapes=[
                pltpu.VMEM((2, group, 128), BF16),
                pltpu.VMEM((2, group, 128), BF16),
                pltpu.VMEM((2, group, 128), BF16),
                pltpu.VMEM((2, group, 128), F32),
                pltpu.VMEM((2, group, 128), F32),
                pltpu.VMEM((2, RUN, RUN), BF16),
                pltpu.VMEM((2, RUN, RUN), BF16),
                pltpu.VMEM((2, group, 128), BF16),
                pltpu.VMEM((2, group, 128), F32),
                pltpu.VMEM((2, group, 128), F32),
                pltpu.VMEM((2, group, 128), F32),
            ],
        ),
        input_output_aliases=alias,
        compiler_params=pltpu.CompilerParams(vmem_limit_bytes=VMEM),
        cost_estimate=SHORT,
        name=f"attend{pair}",
    )(pos, raw, raw, raw, dout, marks, turned, cot, gain_q, gain_k, w_in, w_in, w_in, before, lns, gains)


def combine_body(pos_ref, start_ref, *refs):
    weights, dprojs, atts = refs[0:12], refs[12:15], refs[15:18]
    part_ref, both_s = refs[18:]
    group, width = atts[0].shape[0], weights[3].shape[1]
    bo = sum(dot_nn(atts[p][...], weights[4 * p + 3][...]) for p in range(3))
    both_s[0:group, 0:width] = bo.astype(BF16)
    dn = None
    for p in range(3):
        for n in range(3):
            term = dot_nt(dprojs[p][:, 128 * n : 128 * (n + 1)], weights[4 * p + n][...])
            dn = term if dn is None else dn + term
    both_s[0:group, width : 2 * width] = dn.astype(BF16)
    block = 128
    both_s[group : group + block, :] = both_s[0:block, :]
    back = group - start_ref[0]
    high, rest = back // block, back % block
    row = lax.broadcasted_iota(jnp.int32, (block, 2 * block), 0)
    col = lax.broadcasted_iota(jnp.int32, (block, 2 * block), 1)
    shift = jnp.where(col == row + rest, 1.0, 0.0).astype(BF16)
    half = group // (2 * block)
    for i in range(group // block):
        at = pl.multiple_of(((i + high) % (group // block)) * block, block)
        moved = dot_nn(shift, both_s[pl.ds(at, 2 * block), :]).astype(BF16)
        part_ref[i // half, (i % half) * block : (i % half + 1) * block, :] = moved


def combine(pos, start, w_in, w_attn_out, dprojs, atts):
    group, width = atts[0].shape[0], w_attn_out.shape[1]

    def whole(shape):
        return pl.BlockSpec(shape, lambda i, pos, start: (0,) * len(shape))

    weights, specs = [], []
    for p in range(3):
        for n in range(3):
            weights.append(w_in)
            specs.append(pl.BlockSpec((width, 128), lambda i, pos, start, p=p, n=n: (0, 6 * n + 3 * pos[0] + p)))
        weights.append(w_attn_out)
        specs.append(pl.BlockSpec((128, width), lambda i, pos, start, p=p: (3 * pos[0] + p, 0)))
    out = (2, group // 2, 2 * width)
    return pl.pallas_call(
        combine_body,
        out_shape=jax.ShapeDtypeStruct(out, BF16),
        grid_spec=pltpu.PrefetchScalarGridSpec(
            num_scalar_prefetch=2,
            grid=(1,),
            in_specs=specs + [whole((group, 384))] * 3 + [whole((group, 128))] * 3,
            out_specs=whole(out),
            scratch_shapes=[pltpu.VMEM((group + 128, 2 * width), BF16)],
        ),
        cost_estimate=SHORT,
        compiler_params=pltpu.CompilerParams(vmem_limit_bytes=VMEM),
        name="combine",
    )(pos, start, *weights, *dprojs, *atts)


def finish_body(
    pos_ref, image_ref, cot_ref, gain_ref, here_ref, there_ref, joined_ref, got_ref, out_ref, grad_ref
):
    tokens, width = image_ref.shape
    step = 64
    stays = pos_ref[0] == pos_ref[2]

    def put(source):
        for r in range(0, tokens, step):
            rows = slice(r, r + step)
            x = image_ref[rows, :].astype(F32)
            total = here_ref[rows, :] + (there_ref[rows, :].astype(F32) + source[rows, :].astype(F32))
            out_ref[rows, :] = (x + total[:, 0:width]).astype(BF16)
            center = x - jnp.mean(x, axis=-1, keepdims=True)
            rstd = lax.rsqrt(jnp.mean(center * center, axis=-1, keepdims=True) + EPS)
            scaled = center * rstd
            grad = total[:, width : 2 * width] * gain_ref[...]
            mean = jnp.mean(grad, axis=-1, keepdims=True)
            slope = jnp.mean(grad * scaled, axis=-1, keepdims=True)
            grad_ref[rows, :] = cot_ref[rows, :].astype(F32) + rstd * (grad - mean - scaled * slope)

    pl.when(stays)(lambda: put(joined_ref))
    pl.when(jnp.logical_not(stays))(lambda: put(got_ref))


def finish(pos, image_in, cotangent, ln_gain, here, there, joined, got):
    tokens, width = image_in.shape
    vmem = pl.BlockSpec(memory_space=pltpu.VMEM)
    return pl.pallas_call(
        finish_body,
        out_shape=(jax.ShapeDtypeStruct((tokens, width), BF16), jax.ShapeDtypeStruct((tokens, width), F32)),
        in_specs=[pl.BlockSpec(memory_space=pltpu.SMEM)] + [vmem] * 7,
        out_specs=(vmem, vmem),
        compiler_params=pltpu.CompilerParams(vmem_limit_bytes=VMEM),
        cost_estimate=SHORT,
        name="finish",
    )(pos, image_in, cotangent, ln_gain, here, there, joined, got)


def exchange(value, mask):
    count = lax.axis_size(AXES)
    return lax.ppermute(value, AXES, [(i, i ^ mask) for i in range(count)])


def add_low(left, right):
    return (left.astype(F32) + right.astype(F32)).astype(BF16)


class Order:
    def __init__(self, places):
        self.places = places

    def after(self, value):
        value, self.places = lax.optimization_barrier((value, self.places))
        return value


def reduced(order, halves, masks, rest):
    for mask in masks:
        got = exchange(halves[1], mask)
        yield
        chunk = order.after(add_low(halves[0], order.after(got)))
        middle = chunk.shape[0] // 2
        halves = chunk[:middle], chunk[middle:]
    for mask in rest:
        chunk = order.after(add_low(chunk, exchange(chunk, mask)))
    return chunk


def reduce_only(order, halves, masks, rest):
    yield (yield from reduced(order, halves, masks, rest))


def travel(order, halves, masks, rest):
    chunk = yield from reduced(order, halves, masks, rest)
    for mask in reversed(masks):
        got = exchange(chunk, mask)
        yield
        chunk = order.after(jnp.concatenate([chunk, order.after(got)], axis=0))
    mate = exchange(chunk, 2)
    yield
    yield chunk, order.after(mate)


def spread_mlp_body(pos_ref, all_ref, *refs, masks):
    out_ref, in_ref = refs[-2:]
    rows = all_ref.shape[2] // 2
    side, quarter = pl.program_id(0), pl.program_id(1)
    first = 2 * side + masks[0] * (quarter // 2) + masks[1] * (quarter % 2)
    for i in range(4):
        device = first + masks[2] * (i // 2) + masks[3] * (i % 2)
        out_ref[i * rows : (i + 1) * rows, :] = all_ref[device, 0, 0:rows, :].astype(F32)
        in_ref[i * rows : (i + 1) * rows, :] = all_ref[device, 0, rows : 2 * rows, :].astype(F32)


def spread_mlp(pos, gathered, masks, part, shapes, before):
    devices, _, rows2, width = gathered.shape
    return pl.pallas_call(
        functools.partial(spread_mlp_body, masks=tuple(masks)),
        out_shape=tuple(jax.ShapeDtypeStruct(s, F32) for s in shapes),
        grid_spec=pltpu.PrefetchScalarGridSpec(
            num_scalar_prefetch=1,
            grid=(2, 4),
            in_specs=[pl.BlockSpec((devices, 1, rows2, width), lambda c, g, pos: (0, part, 0, 0))]
            + [pl.BlockSpec(memory_space=pl.ANY)] * len(before),
            out_specs=[
                pl.BlockSpec((width // 4, width), lambda c, g, pos: (4 * (2 * c + part) + g, 0)),
                pl.BlockSpec((width // 4, width), lambda c, g, pos: (g, 3 + 2 * c + part)),
            ],
        ),
        input_output_aliases={2 + i: out for i, out in enumerate(before)},
        compiler_params=pltpu.CompilerParams(dimension_semantics=("arbitrary", "arbitrary"), vmem_limit_bytes=VMEM),
        cost_estimate=SHORT,
        name=f"spread_mlp{part}",
    )(pos, gathered, *before.values())


def spread_attention_body(pos_ref, own_ref, mate_ref, *refs):
    in_ref, out_ref = refs[-3:-1] if own_ref.shape[1] > 64 else refs[-2:]
    sid = pos_ref[1]
    blocks = own_ref.shape[0]
    rows = 48
    side, kind = pl.program_id(0), pl.program_id(2)

    def put(source):
        from_col = pl.ds(pl.multiple_of(128 * kind, 128), 128)
        for i in range(blocks):
            in_ref[i * rows : (i + 1) * rows, :] = source[i ^ sid, 0:rows, from_col].astype(F32)

        @pl.when(kind == 0)
        def _():
            for i in range(blocks):
                piece = source[i ^ sid, rows : rows + 16, :].astype(F32)
                out_ref[8 * i : 8 * (i + 1), 0:384] = piece[0:8]
                out_ref[8 * i : 8 * (i + 1), 384:768] = piece[8:16]

    pl.when(side == 0)(lambda: put(own_ref))
    pl.when(side == 1)(lambda: put(mate_ref))
    if own_ref.shape[1] > 64:
        refs[-1][...] = own_ref[sid, 64:72, :].astype(F32) + mate_ref[sid, 64:72, :].astype(F32)


def spread_attention(pos, own, mate, pairs, shapes, before):
    rows = own.shape[1]
    width = shapes[1][0]
    base = pairs[0]
    block = pl.BlockSpec((BLOCKS, rows, 384), lambda r, p, k, pos: (0, 0, p))
    out_shape = [jax.ShapeDtypeStruct(s, F32) for s in shapes]
    out_specs = [
        pl.BlockSpec((width, 128), lambda r, p, k, pos: (0, 6 * k + 3 * (r ^ pos[0]) + base + p)),
        pl.BlockSpec((128, width), lambda r, p, k, pos: (3 * (r ^ pos[0]) + base + p, 0)),
    ]
    if rows > 64:
        out_shape.append(jax.ShapeDtypeStruct((8, 384), F32))
        out_specs.append(pl.BlockSpec((8, 384), lambda r, p, k, pos: (0, 0)))
    return pl.pallas_call(
        spread_attention_body,
        out_shape=tuple(out_shape),
        grid_spec=pltpu.PrefetchScalarGridSpec(
            num_scalar_prefetch=1,
            grid=(2, len(pairs), 3),
            in_specs=[block, block] + [pl.BlockSpec(memory_space=pl.ANY)] * len(before),
            out_specs=out_specs,
        ),
        input_output_aliases={3 + i: out for i, out in enumerate(before)},
        compiler_params=pltpu.CompilerParams(
            dimension_semantics=("arbitrary",) * 3, vmem_limit_bytes=VMEM
        ),
        cost_estimate=SHORT,
        name=f"spread_attention{base}",
    )(pos, own, mate, *before.values())


def per_device(image_in, ln_gain, w_in, q_gain, k_gain, w_attn_out, w_mlp_out, cotangent, image_ids):
    tokens, width = image_in.shape
    count = lax.axis_size(AXES)
    index = lax.axis_index(AXES)
    side = index & 1
    core = (index >> 1) & 1
    others = [1 << k for k in range(2, count.bit_length() - 1)]
    y, z, far = others[:3]
    masks = {
        "m0": [1, z, far, y],
        "m1": [y, 1, z, far],
        "a0": [1, z, y, far],
        "a1": [y, z, 1, far],
    }
    rest = others[3:]
    crossing = [(i, i ^ 3) for i in range(count) if i & 3 in (1, 2)]

    def place(masks):
        sid = jnp.int32(0)
        for mask in masks:
            sid = 2 * sid + ((index & mask) != 0).astype(jnp.int32)
        return jnp.stack([core, sid, side])

    order = Order({name: place(masks[name]) for name in masks})
    trips, ended = {}, {}

    def chunk(name, keep, send):
        trip = reduce_only if name in ("m0", "m1") else travel
        trips[name] = trip(order, (keep, order.after(send)), masks[name], rest)
        next(trips[name])

    def hop(*names):
        for name in names:
            ended[name] = next(trips[name])

    def call(kernel, name, *values):
        return order.after(kernel(order.places[name], *values))

    gain_row = ln_gain.reshape(1, width)
    gain_q = jnp.concatenate([q_gain, q_gain]).reshape(1, 128)
    gain_k = jnp.concatenate([k_gain, k_gain]).reshape(1, 128)
    ids = lax.dynamic_slice(image_ids, (0, side * tokens), (1, tokens))
    packed = order.after(prep(ids, image_in, cotangent, gain_row))
    beside = exchange(packed, 2)
    crossed = lax.ppermute(packed, AXES, crossing)
    beside = order.after(beside)
    *grads0, here, there, ln0 = call(mlp, "m0", packed, beside, w_in, w_mlp_out, 0, ())
    *grads1, here, there, ln1 = call(mlp, "m1", packed, beside, w_in, w_mlp_out, 1, (here, there))
    swapped = order.after(jnp.where(core == side, packed, order.after(crossed)))
    mate = exchange(swapped, 2)
    chunk("m0", *grads0)
    chunk("m1", *grads1)
    mate = order.after(mate)
    projected = call(project, "a0", swapped, mate, w_in, w_attn_out)
    empty = jnp.zeros((8, 128), BF16)
    sums = (ln0 + ln1, jnp.zeros((16, 128), F32))
    first = call(attend, "a0", 0, projected, gain_q, gain_k, w_in, empty, *sums)
    there = exchange(there, 2)
    hop("m0", "m1")
    second = call(attend, "a0", 1, projected, gain_q, gain_k, w_in, first[0], first[4], first[3])
    chunk("a0", second[0][:8], second[0][8:])
    there = order.after(there)
    hop("m0", "m1")
    third = call(attend, "a1", 2, projected, gain_q, gain_k, w_in, empty, second[4], second[3])
    chunk("a1", third[0][:8], third[0][8:])
    hop("a0", "m0", "m1")
    pieces = (first, second, third)
    parts = call(
        combine, "a0", projected[6], w_in, w_attn_out, [p[1] for p in pieces], [p[2] for p in pieces]
    )
    hop("a0", "a1")
    got = exchange(parts[1], 2)
    hop("m0", "m1")
    gathered = lax.all_gather(order.after(jnp.concatenate([ended["m0"], ended["m1"]])), AXES)
    hop("a0", "a1")
    joined = order.after(add_low(parts[0], order.after(got)))
    got = lax.ppermute(joined, AXES, crossing)
    hop("a0", "a1", "a0", "a1", "a0", "a1")
    got = order.after(got)
    block_out, grad_image = call(
        finish, "a0", image_in, cotangent, gain_row, here, there, joined, got
    )
    hop("a1", "a0", "a1")
    gathered = order.after(gathered)
    of_mlp, of_attention = (w_mlp_out.shape, w_in.shape), (w_in.shape, w_attn_out.shape)
    grad_mlp_w, grad_win = call(spread_mlp, "m0", gathered, masks["m0"], 0, of_mlp, {})
    hop("a1", "a0")
    grad_mlp_w, grad_win = call(spread_mlp, "m1", gathered, masks["m1"], 1, of_mlp, {0: grad_mlp_w, 1: grad_win})
    hop("a1")
    before = {0: grad_win}
    grad_win, grad_attn_w, small = call(spread_attention, "a1", *ended["a1"], (2,), of_attention, before)
    hop("a0")
    before = {0: grad_win, 1: grad_attn_w}
    grad_win, grad_attn_w = call(spread_attention, "a0", *ended["a0"], (0, 1), of_attention, before)
    small = small.reshape(-1)
    return (
        block_out, grad_image, small[0:width] / ln_gain, grad_win, small[width : width + 64],
        small[width + 64 : width + 128], grad_attn_w, grad_mlp_w,
    )


def solution(mesh):
    tokens = P(("seq", "head"), None)
    return jax.shard_map(
        per_device,
        mesh=mesh,
        in_specs=(tokens, P(), P(), P(), P(), P(), P(), tokens, P("seq", None)),
        out_specs=(tokens, tokens, P(), P(), P(), P(), P(), P()),
        check_vma=False,
    )
```

```python
import functools
import math

import jax
import jax.numpy as jnp
from jax import lax
from jax.experimental import pallas as pl
from jax.experimental.pallas import tpu as pltpu
from jax.sharding import PartitionSpec as P

F32 = jnp.float32
BF16 = jnp.bfloat16
EPS = 1e-06
AXES = ("seq", "head")
VMEM = 32 << 20
BLOCKS = 16
EXCLUDE = 32768.0
SHORT = pl.CostEstimate(flops=1, bytes_accessed=1, transcendentals=0)
SCORE_SCALE = 0.125 * math.log2(math.e)


def dot_nn(a, b):
    return lax.dot_general(a, b, (((1,), (0,)), ((), ())), preferred_element_type=F32)


def dot_nt(a, b):
    return lax.dot_general(a, b, (((1,), (1,)), ((), ())), preferred_element_type=F32)


def dot_tn(a, b):
    return lax.dot_general(a, b, (((0,), (0,)), ((), ())), preferred_element_type=F32)


def row_sums(x):
    ones = jnp.ones((8, x.shape[1]), BF16)
    high = x.astype(BF16)
    low = (x - high.astype(F32)).astype(BF16)
    return dot_nt(ones, high) + dot_nt(ones, low)


def prep_body(ids_ref, image_ref, cot_ref, gain_ref, out_ref):
    tokens, width = image_ref.shape
    step = 64
    for r in range(0, tokens, step):
        x = image_ref[r : r + step, :].astype(F32)
        center = x - jnp.mean(x, axis=-1, keepdims=True)
        spread = jnp.mean(center * center, axis=-1, keepdims=True)
        out_ref[r : r + step, 0:width] = (center * lax.rsqrt(spread + EPS) * gain_ref[...]).astype(BF16)
    out_ref[:, width : 2 * width] = cot_ref[...]
    ids = ids_ref[...]
    image = lax.broadcasted_iota(jnp.int32, (128, tokens), 0) & 63
    marks = jnp.where(image == ids, 1.0, 0.0).astype(F32)
    out_ref[:, 2 * width :] = jnp.transpose(marks).astype(BF16)


def prep(ids, image_in, cotangent, ln_gain):
    tokens, width = image_in.shape
    return pl.pallas_call(
        prep_body,
        out_shape=jax.ShapeDtypeStruct((tokens, 2 * width + 128), BF16),
        cost_estimate=SHORT,
        name="prep",
    )(ids, image_in, cotangent, ln_gain)


def mlp_body(
    pos_ref, own_ref, mate_ref, win_ref, wout_ref, *refs,
):
    before = refs[:-11]
    keep_ref, send_ref, here_ref, there_ref, ln_ref, normed_s, cot_s, up_s, dact_s, act_s, dup_s = refs[-11:]
    tokens = own_ref.shape[0]
    width = wout_ref.shape[1]
    sid = pos_ref[1]
    for i, ref in enumerate((own_ref, mate_ref)):
        normed_s[i * tokens : (i + 1) * tokens, :] = ref[:, 0:width]
        cot_s[i * tokens : (i + 1) * tokens, :] = ref[:, width : 2 * width]
    up_s[...] = dot_nn(normed_s[...], win_ref[...])
    dact_s[...] = dot_nt(cot_s[...], wout_ref[...])
    step = 32

    def gelu_rows(i, carry):
        rows = pl.ds(pl.multiple_of(i * step, step), step)
        up = up_s[rows, :]
        cdf = 0.5 * (1.0 + lax.erf(up * math.sqrt(0.5)))
        pdf = jnp.exp(-0.5 * up * up) * (1.0 / math.sqrt(2.0 * math.pi))
        act_s[rows, :] = (up * cdf).astype(BF16)
        dup_s[rows, :] = (dact_s[rows, :] * (cdf + up * pdf)).astype(BF16)
        return carry

    lax.fori_loop(0, 2 * tokens // step, gelu_rows, 0)
    rows = width // BLOCKS
    part = width // 2
    for other, ref in enumerate((keep_ref, send_ref)):
        cols = pl.ds(pl.multiple_of((sid // (BLOCKS // 2) ^ other) * part, part), part)
        grad_out = dot_tn(act_s[:, cols], cot_s[...])
        grad_in = dot_tn(normed_s[:, cols], dup_s[...])
        ln_ref[:, cols] = row_sums(grad_in * win_ref[cols, :].astype(F32))
        for i in range(BLOCKS // 2):
            where = i ^ (sid % (BLOCKS // 2))
            ref[where, 0:rows, :] = grad_out[i * rows : (i + 1) * rows].astype(BF16)
            ref[where, rows : 2 * rows, :] = grad_in[i * rows : (i + 1) * rows].astype(BF16)
    for side in range(2):
        cols = slice(side * width, (side + 1) * width)
        here = dot_nt(dup_s[0:tokens, :], win_ref[...]) if side else dot_nn(act_s[0:tokens, :], wout_ref[...])
        there = dot_nt(dup_s[tokens:, :], win_ref[...]) if side else dot_nn(act_s[tokens:, :], wout_ref[...])
        if before:
            here += before[0][:, cols]
            there += before[1][:, cols].astype(F32)
        here_ref[:, cols] = here
        there_ref[:, cols] = there.astype(BF16)


def mlp(pos, own, mate, w_in, w_mlp_out, part, before):
    tokens = own.shape[0]
    width = w_mlp_out.shape[1]
    rows = width // BLOCKS

    def whole(shape):
        return pl.BlockSpec(shape, lambda i, pos: (0,) * len(shape))

    half = (BLOCKS // 2, 2 * rows, width)
    outs = [half, half, (tokens, 2 * width), (tokens, 2 * width), (8, width)]
    return pl.pallas_call(
        mlp_body,
        out_shape=tuple(jax.ShapeDtypeStruct(s, t) for s, t in zip(outs, (BF16, BF16, F32, BF16, F32))),
        grid_spec=pltpu.PrefetchScalarGridSpec(
            num_scalar_prefetch=1,
            grid=(1,),
            in_specs=[
                whole(own.shape),
                whole(own.shape),
                pl.BlockSpec((width, width), lambda i, pos: (0, 3 + 2 * pos[0] + part)),
                pl.BlockSpec((width, width), lambda i, pos: (2 * pos[0] + part, 0)),
            ]
            + [whole(x.shape) for x in before],
            out_specs=[whole(s) for s in outs],
            scratch_shapes=[pltpu.VMEM((2 * tokens, width), t) for t in (BF16, BF16, F32, F32, BF16, BF16)],
        ),
        compiler_params=pltpu.CompilerParams(dimension_semantics=("arbitrary",), vmem_limit_bytes=54 << 20),
        cost_estimate=SHORT,
        name=f"mlp{part}",
    )(pos, own, mate, w_in, w_mlp_out, *before)


RUN = 768


def project_body(
    pos_ref, own_ref, mate_ref, wq_ref, wk_ref, wv_ref, wo_ref,
    normed_ref, turned_ref, cot_ref, marks_ref, raw_ref, dout_ref, start_ref, twice_s,
):
    tokens, packed = own_ref.shape
    width = wo_ref.shape[1]
    group = 2 * tokens
    block = 128
    twice_s[0:tokens, :] = own_ref[...]
    twice_s[tokens:group, :] = mate_ref[...]
    twice_s[group : group + block, :] = own_ref[0:block, :]
    marks = twice_s[0:group, 2 * width :]
    held = dot_nn(jnp.ones((8, group), BF16), marks)
    lane = lax.broadcasted_iota(jnp.int32, (8, 128), 1)
    chosen = jnp.where(jnp.logical_and(held == float(RUN), lane < 64), 1.0, 0.0).astype(BF16)
    inside = dot_nt(chosen, marks)
    before = pltpu.roll(inside, 1, 1)
    place = lax.broadcasted_iota(jnp.int32, (8, group), 1).astype(F32)
    opens = jnp.where(jnp.logical_and(inside > 0.5, before < 0.5), place, 0.0)
    start = jnp.sum(opens[0:1, :]).astype(jnp.int32)
    start_ref[0] = start
    high, rest = start // block, start % block
    row = lax.broadcasted_iota(jnp.int32, (block, 2 * block), 0)
    col = lax.broadcasted_iota(jnp.int32, (block, 2 * block), 1)
    shift = jnp.where(col == row + rest, 1.0, 0.0).astype(BF16)
    for i in range(group // block):
        at = pl.multiple_of(((i + high) % (group // block)) * block, block)
        moved = dot_nn(shift, twice_s[pl.ds(at, 2 * block), :]).astype(BF16)
        rows = slice(i * block, (i + 1) * block)
        normed_ref[rows, :] = moved[:, 0:width]
        cot_ref[rows, :] = moved[:, width : 2 * width]
        marks_ref[rows, :] = moved[:, 2 * width :]
    for n, w_ref in enumerate((wq_ref, wk_ref, wv_ref)):
        raw_ref[n, :, :] = dot_nn(normed_ref[...], w_ref[...]).astype(BF16)
    dout_ref[...] = dot_nt(cot_ref[...], wo_ref[...]).astype(BF16)
    for j in range(0, width, 128):
        turned_ref[j : j + 128, :] = jnp.transpose(normed_ref[:, j : j + 128].astype(F32)).astype(BF16)


def project(pos, own, mate, w_in, w_attn_out):
    tokens, packed = own.shape
    width = w_attn_out.shape[1]
    group = 2 * tokens
    part = width // 2

    def whole(shape):
        return pl.BlockSpec(shape, lambda i, pos: (0,) * len(shape))

    outs = [(group, width), (width, group), (group, width), (group, 128), (3, group, part), (group, part)]
    return pl.pallas_call(
        project_body,
        out_shape=tuple(jax.ShapeDtypeStruct(s, BF16) for s in outs) + (jax.ShapeDtypeStruct((1,), jnp.int32),),
        grid_spec=pltpu.PrefetchScalarGridSpec(
            num_scalar_prefetch=1,
            grid=(1,),
            in_specs=[
                whole(own.shape),
                whole(own.shape),
                pl.BlockSpec((width, part), lambda i, pos: (0, pos[0])),
                pl.BlockSpec((width, part), lambda i, pos: (0, 2 + pos[0])),
                pl.BlockSpec((width, part), lambda i, pos: (0, 4 + pos[0])),
                pl.BlockSpec((part, width), lambda i, pos: (pos[0], 0)),
            ],
            out_specs=[whole(s) for s in outs] + [pl.BlockSpec(memory_space=pltpu.SMEM)],
            scratch_shapes=[pltpu.VMEM((group + 128, packed), BF16)],
        ),
        cost_estimate=SHORT,
        compiler_params=pltpu.CompilerParams(vmem_limit_bytes=VMEM),
        name="project",
    )(pos, own, mate, w_in, w_in, w_in, w_attn_out)


def split_dot(x, ones):
    high = x.astype(BF16)
    low = (x - high.astype(F32)).astype(BF16)
    return dot_nn(high, ones) + dot_nn(low, ones)


def attend_body(
    pos_ref, q_ref, k_ref, v_ref, dout_ref, marks_ref, turned_ref, cot_ref, gq_ref, gk_ref, wq_ref, wk_ref, wv_ref,
    before_ref, lns_ref, gains_in_ref, grads_ref, dproj_ref, att_ref, gains_ref, ln_ref,
    q_s, k_s, v_s, unit_s, rstd_s, e_s, ds_s, g_s, dq_s, dk_s, dv_s,
):
    group = q_ref.shape[1]
    width = cot_ref.shape[1]
    size = 64
    sid = pos_ref[1]
    step = 256

    def lanes(rows):
        return lax.broadcasted_iota(jnp.int32, (rows, 128), 1)

    same = lax.broadcasted_iota(jnp.int32, (128, 128), 0) // size == lax.broadcasted_iota(jnp.int32, (128, 128), 1) // size
    ones = jnp.where(same, 1.0, 0.0).astype(BF16)

    for r in range(0, group, step):
        rows = slice(r, r + step)
        low = lanes(step) < size
        marks = marks_ref[rows, :].astype(F32)
        away = (marks - 1.0) * EXCLUDE
        v = v_ref[0, rows, :].astype(F32)
        scaled = []
        for n, (raw_ref, gain_ref) in enumerate(((q_ref, gq_ref), (k_ref, gk_ref))):
            raw = raw_ref[0, rows, :]
            center = raw.astype(F32) - dot_nn(raw, ones) * (1.0 / size)
            rstd = lax.rsqrt(split_dot(center * center, ones) * (1.0 / size) + EPS)
            unit = center * rstd
            unit_s[n, rows, :] = unit
            rstd_s[n, rows, :] = rstd
            scaled.append(unit * gain_ref[...])
        for h in range(2):
            mine = low if h == 0 else jnp.logical_not(low)
            q_s[h, rows, :] = jnp.where(mine, scaled[0], marks).astype(BF16)
            k_s[h, rows, :] = jnp.where(mine, scaled[1], away).astype(BF16)
            v_s[h, rows, :] = jnp.where(mine, v, 1.0).astype(BF16)

    block = 256
    for h in range(2):
        for first, count in ((0, RUN), (RUN, group - RUN)):
            span = slice(first, first + count)
            for i in range(0, count, block):
                rows = slice(first + i, first + i + block)
                scores = dot_nt(q_s[h, rows, :], k_s[h, span, :])
                e_s[h, i : i + block, 0:count] = jnp.exp2(scores * SCORE_SCALE).astype(BF16)
            for i in range(0, count, block):
                rows = slice(first + i, first + i + block)
                lane = lanes(block)
                mine = (lane < size) if h == 0 else (lane >= size)
                spare = size if h == 0 else 0
                outs = dot_nn(e_s[h, i : i + block, 0:count], v_s[h, span, :])
                inverse = 1.0 / pltpu.roll(outs, size, 1)
                attended = outs * inverse
                grad_low = (dout_ref[rows, :].astype(F32) * inverse).astype(BF16).astype(F32)
                centre = split_dot(jnp.where(mine, grad_low * attended, 0.0), jnp.ones((128, 128), BF16))
                centre_high = centre.astype(BF16).astype(F32)
                extra = jnp.where(lane == spare, -centre_high, jnp.where(lane == spare + 1, centre_high - centre, 0.0))
                grad_ext = jnp.where(mine, grad_low, extra).astype(BF16)
                g_s[h, rows, :] = grad_ext
                if h == 0:
                    att_ref[rows, :] = attended.astype(BF16)
                else:
                    att_ref[rows, :] = jnp.where(mine, attended, att_ref[rows, :].astype(F32)).astype(BF16)
                d_probs = dot_nt(grad_ext, v_s[h, span, :])
                ds_s[h, i : i + block, 0:count] = (e_s[h, i : i + block, 0:count].astype(F32) * d_probs).astype(BF16)
            dq_s[h, span, :] = dot_nn(ds_s[h, 0:count, 0:count], k_s[h, span, :])
            dk_s[h, span, :] = dot_tn(ds_s[h, 0:count, 0:count], q_s[h, span, :])
            dv_s[h, span, :] = dot_tn(e_s[h, 0:count, 0:count], g_s[h, span, :])

    for r in range(0, group, step):
        rows = slice(r, r + step)
        low = lanes(step) < size
        for n, (grad_s, gain_ref) in enumerate(((dq_s, gq_ref), (dk_s, gk_ref))):
            unit, rstd = unit_s[n, rows, :], rstd_s[n, rows, :]
            grad = jnp.where(low, grad_s[0, rows, :], grad_s[1, rows, :]) * 0.125
            part = jnp.sum((grad * unit).reshape(step // 8, 8, 128), axis=0)
            if r == 0:
                gains_ref[8 * n : 8 * (n + 1), :] = gains_in_ref[8 * n : 8 * (n + 1), :] + part
            else:
                gains_ref[8 * n : 8 * (n + 1), :] += part
            grad = grad * gain_ref[...]
            mean = split_dot(grad, ones) * (1.0 / size)
            slope = split_dot(grad * unit, ones) * (1.0 / size)
            dproj_ref[rows, 128 * n : 128 * (n + 1)] = (rstd * (grad - mean - unit * slope)).astype(BF16)
        dproj_ref[rows, 256:384] = jnp.where(low, dv_s[0, rows, :], dv_s[1, rows, :]).astype(BF16)

    rows = width // BLOCKS
    part = 384
    for j in range(0, width, part):
        grad_in = dot_nn(turned_ref[j : j + part, :], dproj_ref[...])
        terms = lns_ref[:, j : j + part]
        for n, w_ref in enumerate((wq_ref, wk_ref, wv_ref)):
            terms += row_sums(grad_in[:, 128 * n : 128 * (n + 1)] * w_ref[j : j + part, :].astype(F32))
        ln_ref[:, j : j + part] = terms
        for i in range(part // rows):
            grads_ref[(j // rows + i) ^ sid, 0:rows, :] = grad_in[i * rows : (i + 1) * rows].astype(BF16)
    grad_out = dot_tn(att_ref[...], cot_ref[...])
    few = 128 // BLOCKS
    for i in range(BLOCKS):
        piece = grad_out[i * few : (i + 1) * few]
        piece = jnp.concatenate([piece[:, :384], piece[:, 384:]], axis=0)
        grads_ref[i ^ sid, rows : rows + 2 * few, :] = piece.astype(BF16)
    rows += 2 * few
    if grads_ref.shape[1] > rows:
        gains = jnp.sum(gains_ref[...].reshape(2, 8, 128), axis=1)
        gains = gains + pltpu.roll(gains, size, 1)
        gains = jnp.where(lanes(1) < size, gains[0:1], gains[1:2])
        small = [ln_ref[0:1, 0:384], ln_ref[0:1, 384:768], jnp.concatenate([gains, jnp.zeros((1, 256), F32)], axis=1)]
        small = jnp.concatenate(small + [jnp.zeros((5, 384), F32)], axis=0)
        for i in range(BLOCKS):
            grads_ref[i ^ sid, rows : rows + 8, :] = (small if i == 0 else jnp.zeros_like(small)).astype(BF16)


def attend(pos, pair, projected, gain_q, gain_k, w_in, before, lns, gains):
    normed, turned, cot, marks, raw, dout, _ = projected
    group, width = normed.shape
    last = pair == 2
    rows = width // BLOCKS + 16 + 8 * last
    cols = 384 if last else 768
    alias = {13: 0} if pair == 1 else {}
    before_spec = pl.BlockSpec(memory_space=pl.ANY)

    def whole(shape):
        return pl.BlockSpec(shape, lambda i, pos: (0,) * len(shape))

    raw_specs = [pl.BlockSpec((1, group, 128), lambda i, pos, n=n: (n, 0, pair)) for n in range(3)]
    return pl.pallas_call(
        attend_body,
        out_shape=(
            jax.ShapeDtypeStruct((BLOCKS, rows, cols), BF16),
            jax.ShapeDtypeStruct((group, 384), BF16),
            jax.ShapeDtypeStruct((group, 128), BF16),
            jax.ShapeDtypeStruct((16, 128), F32),
            jax.ShapeDtypeStruct((8, width), F32),
        ),
        grid_spec=pltpu.PrefetchScalarGridSpec(
            num_scalar_prefetch=1,
            grid=(1,),
            in_specs=raw_specs
            + [
                pl.BlockSpec((group, 128), lambda i, pos: (0, pair)),
                whole(marks.shape),
                whole(turned.shape),
                whole(cot.shape),
                whole((1, 128)),
                whole((1, 128)),
            ]
            + [pl.BlockSpec((width, 128), lambda i, pos, n=n: (0, 6 * n + 3 * pos[0] + pair)) for n in range(3)]
            + [before_spec, whole((8, width)), whole((16, 128))],
            out_specs=[
                pl.BlockSpec((BLOCKS, rows, 384), lambda i, pos: (0, 0, 1 if pair == 1 else 0)),
                whole((group, 384)),
                whole((group, 128)),
                whole((16, 128)),
                whole((8, width)),
            ],
            scratch_shapes=[
                pltpu.VMEM((2, group, 128), BF16),
                pltpu.VMEM((2, group, 128), BF16),
                pltpu.VMEM((2, group, 128), BF16),
                pltpu.VMEM((2, group, 128), F32),
                pltpu.VMEM((2, group, 128), F32),
                pltpu.VMEM((2, RUN, RUN), BF16),
                pltpu.VMEM((2, RUN, RUN), BF16),
                pltpu.VMEM((2, group, 128), BF16),
                pltpu.VMEM((2, group, 128), F32),
                pltpu.VMEM((2, group, 128), F32),
                pltpu.VMEM((2, group, 128), F32),
            ],
        ),
        input_output_aliases=alias,
        compiler_params=pltpu.CompilerParams(vmem_limit_bytes=VMEM),
        cost_estimate=SHORT,
        name=f"attend{pair}",
    )(pos, raw, raw, raw, dout, marks, turned, cot, gain_q, gain_k, w_in, w_in, w_in, before, lns, gains)


def combine_body(pos_ref, start_ref, *refs):
    weights, dprojs, atts = refs[0:12], refs[12:15], refs[15:18]
    part_ref, both_s = refs[18:]
    group, width = atts[0].shape[0], weights[3].shape[1]
    bo = sum(dot_nn(atts[p][...], weights[4 * p + 3][...]) for p in range(3))
    both_s[0:group, 0:width] = bo.astype(BF16)
    dn = None
    for p in range(3):
        for n in range(3):
            term = dot_nt(dprojs[p][:, 128 * n : 128 * (n + 1)], weights[4 * p + n][...])
            dn = term if dn is None else dn + term
    both_s[0:group, width : 2 * width] = dn.astype(BF16)
    block = 128
    both_s[group : group + block, :] = both_s[0:block, :]
    back = group - start_ref[0]
    high, rest = back // block, back % block
    row = lax.broadcasted_iota(jnp.int32, (block, 2 * block), 0)
    col = lax.broadcasted_iota(jnp.int32, (block, 2 * block), 1)
    shift = jnp.where(col == row + rest, 1.0, 0.0).astype(BF16)
    half = group // (2 * block)
    for i in range(group // block):
        at = pl.multiple_of(((i + high) % (group // block)) * block, block)
        moved = dot_nn(shift, both_s[pl.ds(at, 2 * block), :]).astype(BF16)
        part_ref[i // half, (i % half) * block : (i % half + 1) * block, :] = moved


def combine(pos, start, w_in, w_attn_out, dprojs, atts):
    group, width = atts[0].shape[0], w_attn_out.shape[1]

    def whole(shape):
        return pl.BlockSpec(shape, lambda i, pos, start: (0,) * len(shape))

    weights, specs = [], []
    for p in range(3):
        for n in range(3):
            weights.append(w_in)
            specs.append(pl.BlockSpec((width, 128), lambda i, pos, start, p=p, n=n: (0, 6 * n + 3 * pos[0] + p)))
        weights.append(w_attn_out)
        specs.append(pl.BlockSpec((128, width), lambda i, pos, start, p=p: (3 * pos[0] + p, 0)))
    out = (2, group // 2, 2 * width)
    return pl.pallas_call(
        combine_body,
        out_shape=jax.ShapeDtypeStruct(out, BF16),
        grid_spec=pltpu.PrefetchScalarGridSpec(
            num_scalar_prefetch=2,
            grid=(1,),
            in_specs=specs + [whole((group, 384))] * 3 + [whole((group, 128))] * 3,
            out_specs=whole(out),
            scratch_shapes=[pltpu.VMEM((group + 128, 2 * width), BF16)],
        ),
        cost_estimate=SHORT,
        compiler_params=pltpu.CompilerParams(vmem_limit_bytes=VMEM),
        name="combine",
    )(pos, start, *weights, *dprojs, *atts)


def finish_body(
    pos_ref, image_ref, cot_ref, gain_ref, here_ref, there_ref, joined_ref, got_ref, out_ref, grad_ref
):
    tokens, width = image_ref.shape
    step = 64
    stays = pos_ref[0] == pos_ref[2]

    def put(source):
        for r in range(0, tokens, step):
            rows = slice(r, r + step)
            x = image_ref[rows, :].astype(F32)
            total = here_ref[rows, :] + (there_ref[rows, :].astype(F32) + source[rows, :].astype(F32))
            out_ref[rows, :] = (x + total[:, 0:width]).astype(BF16)
            center = x - jnp.mean(x, axis=-1, keepdims=True)
            rstd = lax.rsqrt(jnp.mean(center * center, axis=-1, keepdims=True) + EPS)
            scaled = center * rstd
            grad = total[:, width : 2 * width] * gain_ref[...]
            mean = jnp.mean(grad, axis=-1, keepdims=True)
            slope = jnp.mean(grad * scaled, axis=-1, keepdims=True)
            grad_ref[rows, :] = cot_ref[rows, :].astype(F32) + rstd * (grad - mean - scaled * slope)

    pl.when(stays)(lambda: put(joined_ref))
    pl.when(jnp.logical_not(stays))(lambda: put(got_ref))


def finish(pos, image_in, cotangent, ln_gain, here, there, joined, got):
    tokens, width = image_in.shape
    vmem = pl.BlockSpec(memory_space=pltpu.VMEM)
    return pl.pallas_call(
        finish_body,
        out_shape=(jax.ShapeDtypeStruct((tokens, width), BF16), jax.ShapeDtypeStruct((tokens, width), F32)),
        in_specs=[pl.BlockSpec(memory_space=pltpu.SMEM)] + [vmem] * 7,
        out_specs=(vmem, vmem),
        compiler_params=pltpu.CompilerParams(vmem_limit_bytes=VMEM),
        cost_estimate=SHORT,
        name="finish",
    )(pos, image_in, cotangent, ln_gain, here, there, joined, got)


def exchange(value, mask):
    count = lax.axis_size(AXES)
    return lax.ppermute(value, AXES, [(i, i ^ mask) for i in range(count)])


def add_low(left, right):
    return (left.astype(F32) + right.astype(F32)).astype(BF16)


class Order:
    def __init__(self, places):
        self.places = places

    def after(self, value):
        value, self.places = lax.optimization_barrier((value, self.places))
        return value


def reduced(order, halves, masks, rest):
    for mask in masks:
        got = exchange(halves[1], mask)
        yield
        chunk = order.after(add_low(halves[0], order.after(got)))
        middle = chunk.shape[0] // 2
        halves = chunk[:middle], chunk[middle:]
    for mask in rest:
        chunk = order.after(add_low(chunk, exchange(chunk, mask)))
    return chunk


def reduce_only(order, halves, masks, rest):
    yield (yield from reduced(order, halves, masks, rest))


def travel(order, halves, masks, rest):
    chunk = yield from reduced(order, halves, masks, rest)
    for mask in reversed(masks):
        got = exchange(chunk, mask)
        yield
        chunk = order.after(jnp.concatenate([chunk, order.after(got)], axis=0))
    mate = exchange(chunk, 2)
    yield
    yield chunk, order.after(mate)


def spread_mlp_body(pos_ref, all_ref, *refs, masks):
    out_ref, in_ref = refs[-2:]
    rows = all_ref.shape[2] // 2
    side, quarter = pl.program_id(0), pl.program_id(1)
    first = 2 * side + masks[0] * (quarter // 2) + masks[1] * (quarter % 2)
    for i in range(4):
        device = first + masks[2] * (i // 2) + masks[3] * (i % 2)
        out_ref[i * rows : (i + 1) * rows, :] = all_ref[device, 0, 0:rows, :].astype(F32)
        in_ref[i * rows : (i + 1) * rows, :] = all_ref[device, 0, rows : 2 * rows, :].astype(F32)


def spread_mlp(pos, gathered, masks, part, shapes, before):
    devices, _, rows2, width = gathered.shape
    return pl.pallas_call(
        functools.partial(spread_mlp_body, masks=tuple(masks)),
        out_shape=tuple(jax.ShapeDtypeStruct(s, F32) for s in shapes),
        grid_spec=pltpu.PrefetchScalarGridSpec(
            num_scalar_prefetch=1,
            grid=(2, 4),
            in_specs=[pl.BlockSpec((devices, 1, rows2, width), lambda c, g, pos: (0, part, 0, 0))]
            + [pl.BlockSpec(memory_space=pl.ANY)] * len(before),
            out_specs=[
                pl.BlockSpec((width // 4, width), lambda c, g, pos: (4 * (2 * c + part) + g, 0)),
                pl.BlockSpec((width // 4, width), lambda c, g, pos: (g, 3 + 2 * c + part)),
            ],
        ),
        input_output_aliases={2 + i: out for i, out in enumerate(before)},
        compiler_params=pltpu.CompilerParams(dimension_semantics=("arbitrary", "arbitrary"), vmem_limit_bytes=VMEM),
        cost_estimate=SHORT,
        name=f"spread_mlp{part}",
    )(pos, gathered, *before.values())


def spread_attention_body(pos_ref, own_ref, mate_ref, *refs):
    in_ref, out_ref = refs[-3:-1] if own_ref.shape[1] > 64 else refs[-2:]
    sid = pos_ref[1]
    blocks = own_ref.shape[0]
    rows = 48
    side, kind = pl.program_id(0), pl.program_id(2)

    def put(source):
        from_col = pl.ds(pl.multiple_of(128 * kind, 128), 128)
        for i in range(blocks):
            in_ref[i * rows : (i + 1) * rows, :] = source[i ^ sid, 0:rows, from_col].astype(F32)

        @pl.when(kind == 0)
        def _():
            for i in range(blocks):
                piece = source[i ^ sid, rows : rows + 16, :].astype(F32)
                out_ref[8 * i : 8 * (i + 1), 0:384] = piece[0:8]
                out_ref[8 * i : 8 * (i + 1), 384:768] = piece[8:16]

    pl.when(side == 0)(lambda: put(own_ref))
    pl.when(side == 1)(lambda: put(mate_ref))
    if own_ref.shape[1] > 64:
        refs[-1][...] = own_ref[sid, 64:72, :].astype(F32) + mate_ref[sid, 64:72, :].astype(F32)


def spread_attention(pos, own, mate, pairs, shapes, before):
    rows = own.shape[1]
    width = shapes[1][0]
    base = pairs[0]
    block = pl.BlockSpec((BLOCKS, rows, 384), lambda r, p, k, pos: (0, 0, p))
    out_shape = [jax.ShapeDtypeStruct(s, F32) for s in shapes]
    out_specs = [
        pl.BlockSpec((width, 128), lambda r, p, k, pos: (0, 6 * k + 3 * (r ^ pos[0]) + base + p)),
        pl.BlockSpec((128, width), lambda r, p, k, pos: (3 * (r ^ pos[0]) + base + p, 0)),
    ]
    if rows > 64:
        out_shape.append(jax.ShapeDtypeStruct((8, 384), F32))
        out_specs.append(pl.BlockSpec((8, 384), lambda r, p, k, pos: (0, 0)))
    return pl.pallas_call(
        spread_attention_body,
        out_shape=tuple(out_shape),
        grid_spec=pltpu.PrefetchScalarGridSpec(
            num_scalar_prefetch=1,
            grid=(2, len(pairs), 3),
            in_specs=[block, block] + [pl.BlockSpec(memory_space=pl.ANY)] * len(before),
            out_specs=out_specs,
        ),
        input_output_aliases={3 + i: out for i, out in enumerate(before)},
        compiler_params=pltpu.CompilerParams(
            dimension_semantics=("arbitrary",) * 3, vmem_limit_bytes=VMEM
        ),
        cost_estimate=SHORT,
        name=f"spread_attention{base}",
    )(pos, own, mate, *before.values())


def per_device(image_in, ln_gain, w_in, q_gain, k_gain, w_attn_out, w_mlp_out, cotangent, image_ids):
    tokens, width = image_in.shape
    count = lax.axis_size(AXES)
    index = lax.axis_index(AXES)
    side = index & 1
    core = (index >> 1) & 1
    others = [1 << k for k in range(2, count.bit_length() - 1)]
    y, z, far = others[:3]
    masks = {
        "m0": [1, z, far, y],
        "m1": [y, 1, z, far],
        "a0": [1, z, y, far],
        "a1": [y, z, 1, far],
    }
    rest = others[3:]
    crossing = [(i, i ^ 3) for i in range(count) if i & 3 in (1, 2)]

    def place(masks):
        sid = jnp.int32(0)
        for mask in masks:
            sid = 2 * sid + ((index & mask) != 0).astype(jnp.int32)
        return jnp.stack([core, sid, side])

    order = Order({name: place(masks[name]) for name in masks})
    trips, ended = {}, {}

    def chunk(name, keep, send):
        trip = reduce_only if name in ("m0", "m1") else travel
        trips[name] = trip(order, (keep, order.after(send)), masks[name], rest)
        next(trips[name])

    def hop(*names):
        for name in names:
            ended[name] = next(trips[name])

    def call(kernel, name, *values):
        return order.after(kernel(order.places[name], *values))

    gain_row = ln_gain.reshape(1, width)
    gain_q = jnp.concatenate([q_gain, q_gain]).reshape(1, 128)
    gain_k = jnp.concatenate([k_gain, k_gain]).reshape(1, 128)
    ids = lax.dynamic_slice(image_ids, (0, side * tokens), (1, tokens))
    packed = order.after(prep(ids, image_in, cotangent, gain_row))
    beside = exchange(packed, 2)
    crossed = lax.ppermute(packed, AXES, crossing)
    beside = order.after(beside)
    *grads0, here, there, ln0 = call(mlp, "m0", packed, beside, w_in, w_mlp_out, 0, ())
    *grads1, here, there, ln1 = call(mlp, "m1", packed, beside, w_in, w_mlp_out, 1, (here, there))
    swapped = order.after(jnp.where(core == side, packed, order.after(crossed)))
    mate = exchange(swapped, 2)
    chunk("m0", *grads0)
    chunk("m1", *grads1)
    mate = order.after(mate)
    projected = call(project, "a0", swapped, mate, w_in, w_attn_out)
    empty = jnp.zeros((8, 128), BF16)
    sums = (ln0 + ln1, jnp.zeros((16, 128), F32))
    first = call(attend, "a0", 0, projected, gain_q, gain_k, w_in, empty, *sums)
    there = exchange(there, 2)
    hop("m0", "m1")
    second = call(attend, "a0", 1, projected, gain_q, gain_k, w_in, first[0], first[4], first[3])
    chunk("a0", second[0][:8], second[0][8:])
    there = order.after(there)
    hop("m0", "m1")
    third = call(attend, "a1", 2, projected, gain_q, gain_k, w_in, empty, second[4], second[3])
    chunk("a1", third[0][:8], third[0][8:])
    hop("a0", "m0", "m1")
    pieces = (first, second, third)
    parts = call(
        combine, "a0", projected[6], w_in, w_attn_out, [p[1] for p in pieces], [p[2] for p in pieces]
    )
    hop("a0", "a1")
    got = exchange(parts[1], 2)
    hop("m0", "m1")
    gathered = lax.all_gather(order.after(jnp.concatenate([ended["m0"], ended["m1"]])), AXES)
    hop("a0", "a1")
    joined = order.after(add_low(parts[0], order.after(got)))
    hop("a0", "a1")
    got = lax.ppermute(joined, AXES, crossing)
    hop("a0", "a1", "a0", "a1")
    got = order.after(got)
    block_out, grad_image = call(
        finish, "a0", image_in, cotangent, gain_row, here, there, joined, got
    )
    hop("a1", "a0", "a1")
    gathered = order.after(gathered)
    of_mlp, of_attention = (w_mlp_out.shape, w_in.shape), (w_in.shape, w_attn_out.shape)
    grad_mlp_w, grad_win = call(spread_mlp, "m0", gathered, masks["m0"], 0, of_mlp, {})
    hop("a1", "a0")
    grad_mlp_w, grad_win = call(spread_mlp, "m1", gathered, masks["m1"], 1, of_mlp, {0: grad_mlp_w, 1: grad_win})
    hop("a1")
    before = {0: grad_win}
    grad_win, grad_attn_w, small = call(spread_attention, "a1", *ended["a1"], (2,), of_attention, before)
    hop("a0")
    before = {0: grad_win, 1: grad_attn_w}
    grad_win, grad_attn_w = call(spread_attention, "a0", *ended["a0"], (0, 1), of_attention, before)
    small = small.reshape(-1)
    return (
        block_out, grad_image, small[0:width] / ln_gain, grad_win, small[width : width + 64],
        small[width + 64 : width + 128], grad_attn_w, grad_mlp_w,
    )


def solution(mesh):
    tokens = P(("seq", "head"), None)
    return jax.shard_map(
        per_device,
        mesh=mesh,
        in_specs=(tokens, P(), P(), P(), P(), P(), P(), tokens, P("seq", None)),
        out_specs=(tokens, tokens, P(), P(), P(), P(), P(), P()),
        check_vma=False,
    )
```
